32 devices in a mesh: groups: 2 (over y), ctx: 16 (over z, x, core).
Axes of the slice: x: 2, y: 2, z: 4, core: 2. Of those that a mesh axis runs over, the one named last changes fastest.
Arguments:
- query_rows: bfloat16 [4096, 2560], P(('groups', 'ctx')), parts along dimension 0, may hold values from -211 to 211
- key_rows: bfloat16 [4096, 2560], P(('groups', 'ctx')), parts along dimension 0, may hold values from -6.2 to 6.2
- value_rows: bfloat16 [4096, 2560], P(('groups', 'ctx')), parts along dimension 0, may hold values from -6 to 6
- out_grad: bfloat16 [4096, 2560], P(('groups', 'ctx')), parts along dimension 0, may hold values from -6 to 6
- selected: int32 [32, 8], P('groups'), parts along dimension 0, may hold values from 0 to 15, as said below
Outputs:
- attended: bfloat16 [4096, 2560], P(('groups', 'ctx')), parts along dimension 0
- grad_query: bfloat16 [4096, 2560], P(('groups', 'ctx')), parts along dimension 0
- grad_key: bfloat16 [4096, 2560], P(('groups', 'ctx')), parts along dimension 0
- grad_value: bfloat16 [4096, 2560], P(('groups', 'ctx')), parts along dimension 0
- pooled_key_grad: float32 [64, 2560], P(('groups', 'ctx')), parts along dimension 0
- pooled_value_grad: float32 [64, 2560], P(('groups', 'ctx')), parts along dimension 0
The draws below stay inside these ranges and needn't reach their ends.
There are 2 independent parts, one for each index of `groups`. The reference program is written for one: setup_inputs(seed, part) draws one part's arguments, and reference() takes and returns one part's arrays. A program takes and returns all parts, laid end to end along the dimension named above; each array names one. Nothing has to cross between parts.
Inputs may be any that keep to these rules, and one draw needn't show every extreme that they name: `selected`: each row names 8 different tiles.
All inputs are finite; a program needn't handle non-finite values.
Results may differ from the reference program's by a relative error of at most 0.029.
Values may be sent and summed in bfloat16 or wider, within the bound.
A program may use at most 192 MiB of HBM per device.

```python
import jax
import jax.numpy as jnp
from jax import lax

HEADS = 20
HEAD_DIM = 128
TILE = 128
POOL = 64
SEL = 8
TILES = 16
TOKENS = 2048
COMP = 32


def draw_selected(key, part):
    seeded = jax.random.fold_in(key, 101)
    popular = jax.random.randint(jax.random.fold_in(seeded, 1), (TILES,), 0, 4)
    jitter = jax.random.randint(jax.random.fold_in(seeded, 2), (TILES, TILES), 0, 4096)
    tile_ids = jnp.arange(TILES, dtype=jnp.int32)
    order = jax.random.permutation(jax.random.fold_in(seeded, 3), TILES).astype(jnp.int32)
    place = jnp.zeros((TILES,), jnp.int32).at[order].set(tile_ids)
    offset = (place[None, :] - tile_ids[:, None]) % TILES
    base = (offset < SEL // 2).astype(jnp.int32)
    ranking = (jitter + 1024 * popular[None, :] + 16384 * base) * TILES + tile_ids[None, :]
    return lax.top_k(ranking, SEL)[1].astype(jnp.int32)


def block_rows(key, stamp):
    columns = HEADS * HEAD_DIM
    common = jax.random.normal(jax.random.fold_in(key, stamp), (COMP, 1, columns), jnp.float32)
    jitter = jax.random.normal(jax.random.fold_in(key, stamp + 1), (COMP, POOL, columns), jnp.float32)
    return jnp.clip((common + jitter) * 0.7071, -6.0, 6.0).reshape(TOKENS, columns)


def draw_key_rows(key, part):
    result = block_rows(key, 201)
    return jnp.clip(result, -6.2, 6.2).astype(jnp.bfloat16)


def draw_query_rows(key, part):
    columns = HEADS * HEAD_DIM
    result = jnp.clip(1.5 * jax.random.normal(jax.random.fold_in(key, 401), (TOKENS, columns), jnp.float32), -8.0, 8.0)
    return result.astype(jnp.bfloat16)


def draw_value_rows(key, part):
    return block_rows(key, 301).astype(jnp.bfloat16)


def draw_out_grad(key, part):
    columns = HEADS * HEAD_DIM
    result = jax.random.normal(jax.random.fold_in(key, 502), (TOKENS, columns), jnp.float32)
    return jnp.clip(result, -6.0, 6.0).astype(jnp.bfloat16)


def setup_inputs(seed: int = 0, part: int = 0) -> dict:
    key_list = jax.random.split(jax.random.key(seed), 6)
    part_splits = jax.random.split(jax.random.fold_in(key_list[5], part), 6)
    return {
        "query_rows": draw_query_rows(jax.random.fold_in(jax.random.fold_in(key_list[5], part), 71), part),
        "key_rows": draw_key_rows(jax.random.fold_in(jax.random.fold_in(key_list[5], part), 71), part),
        "value_rows": draw_value_rows(jax.random.fold_in(jax.random.fold_in(key_list[5], part), 71), part),
        "out_grad": draw_out_grad(jax.random.fold_in(jax.random.fold_in(key_list[5], part), 71), part),
        "selected": draw_selected(jax.random.fold_in(jax.random.fold_in(key_list[5], part), 71), part),
    }


def pooled(rows):
    return jnp.mean(rows.astype(jnp.float32).reshape(-1, POOL, rows.shape[1]), axis=1).astype(jnp.bfloat16)


def settle(array):
    return lax.optimization_barrier(array.astype(jnp.bfloat16)).astype(jnp.float32)


def tile_pass(queries, grads_out, keys_all, values_all):
    scaling = HEAD_DIM ** -0.5
    height = queries.shape[0]
    key_count = keys_all.shape[0]
    columns = HEADS * HEAD_DIM
    highest = lax.Precision.HIGHEST
    head_query = queries.astype(jnp.float32).reshape(height, HEADS, HEAD_DIM)
    head_grad = grads_out.astype(jnp.float32).reshape(height, HEADS, HEAD_DIM)
    head_key = keys_all.astype(jnp.float32).reshape(key_count, HEADS, HEAD_DIM)
    head_value = values_all.astype(jnp.float32).reshape(key_count, HEADS, HEAD_DIM)
    scores = jnp.einsum("rhd,khd->hrk", head_query, head_key, precision=highest) * scaling
    summit = jnp.max(scores, axis=-1, keepdims=True)
    raised = jnp.exp(scores - summit)
    weights = raised / jnp.sum(raised, axis=-1, keepdims=True)
    rounded = settle(weights)
    attended = jnp.einsum("hrk,khd->rhd", rounded, head_value, precision=highest).astype(jnp.bfloat16)
    row_dots = jnp.sum(head_grad * attended.astype(jnp.float32), axis=-1)
    prob_grad = jnp.einsum("rhd,khd->hrk", head_grad, head_value, precision=highest)
    score_grad = settle(weights * (prob_grad - row_dots.T[:, :, None]))
    grad_query = (jnp.einsum("hrk,khd->rhd", score_grad, head_key, precision=highest) * scaling).astype(jnp.bfloat16)
    key_terms = jnp.einsum("hrk,rhd->khd", score_grad, head_query, precision=highest) * scaling
    value_terms = jnp.einsum("hrk,rhd->khd", rounded, head_grad, precision=highest)
    return (attended.reshape(height, columns), grad_query.reshape(height, columns),
            key_terms.reshape(key_count, columns), value_terms.reshape(key_count, columns))


def reference(query_rows, key_rows, value_rows, out_grad, selected):
    columns = HEADS * HEAD_DIM
    pool_keys = pooled(key_rows)
    pool_values = pooled(value_rows)
    key_tiles = key_rows.reshape(TILES, TILE, columns)
    value_tiles = value_rows.reshape(TILES, TILE, columns)

    def advance(totals, inputs):
        coarse_keys, coarse_values, fine_keys, fine_values = totals
        queries, grads_out, listed = inputs
        keys_all = jnp.concatenate([pool_keys, key_tiles[listed].reshape(SEL * TILE, columns)], axis=0)
        values_all = jnp.concatenate([pool_values, value_tiles[listed].reshape(SEL * TILE, columns)], axis=0)
        attended, grad_query, key_terms, value_terms = tile_pass(queries, grads_out, keys_all, values_all)
        coarse_keys = coarse_keys + key_terms[:COMP]
        coarse_values = coarse_values + value_terms[:COMP]
        fine_keys = fine_keys.at[listed].add(settle(key_terms[COMP:]).reshape(SEL, TILE, columns))
        fine_values = fine_values.at[listed].add(settle(value_terms[COMP:]).reshape(SEL, TILE, columns))
        return (coarse_keys, coarse_values, fine_keys, fine_values), (attended, grad_query)

    initial = (jnp.zeros((COMP, columns), jnp.float32), jnp.zeros((COMP, columns), jnp.float32),
               jnp.zeros((TILES, TILE, columns), jnp.float32), jnp.zeros((TILES, TILE, columns), jnp.float32))
    totals, outputs = lax.scan(advance, initial, (query_rows.reshape(TILES, TILE, columns),
                                                  out_grad.reshape(TILES, TILE, columns), selected))
    coarse_keys, coarse_values, fine_keys, fine_values = totals
    attended = outputs[0].reshape(TOKENS, columns)
    grad_query = outputs[1].reshape(TOKENS, columns)
    grad_key = (settle(fine_keys.reshape(TOKENS, columns)) + jnp.repeat(coarse_keys, POOL, axis=0) / POOL).astype(jnp.bfloat16)
    grad_value = (settle(fine_values.reshape(TOKENS, columns)) + jnp.repeat(coarse_values, POOL, axis=0) / POOL).astype(jnp.bfloat16)
    return (attended, grad_query, grad_key, grad_value, coarse_keys, coarse_values)
```

```python
import functools
import math

import jax
import jax.numpy as jnp
from jax import lax
from jax.experimental import pallas as pl
from jax.experimental.pallas import tpu as pltpu
from jax.sharding import PartitionSpec as P

HEADS = 20
HEAD_DIM = 128
TILE = 128
POOL = 64
SEL = 8
CORES = 2
PAIR = 2


def pooled(rows):
    return jnp.mean(rows.astype(jnp.float32).reshape(-1, POOL, rows.shape[1]), axis=1).astype(
        jnp.bfloat16
    )


def contract(left, right, left_dim, right_dim):
    return lax.dot_general(
        left, right, (((left_dim,), (right_dim,)), ((), ())), preferred_element_type=jnp.float32
    )


def attend(queries, grads_out, keys_all, values_all):
    scaling = HEAD_DIM ** (-0.5)
    out_parts, query_parts, key_parts, value_parts = ([], [], [], [])
    for head in range(HEADS):
        lower = head * HEAD_DIM
        upper = lower + HEAD_DIM
        head_query = queries[:, lower:upper]
        head_grad = grads_out[:, lower:upper]
        head_key = keys_all[:, lower:upper]
        head_value = values_all[:, lower:upper]
        scores = contract(head_query, head_key, 1, 1) * scaling
        summit = jnp.max(scores, axis=-1, keepdims=True)
        raised = jnp.exp(scores - summit)
        weights = raised / jnp.sum(raised, axis=-1, keepdims=True)
        rounded = weights.astype(jnp.bfloat16)
        out_rows = jnp.dot(rounded, head_value, preferred_element_type=jnp.float32).astype(
            jnp.bfloat16
        )
        row_dots = jnp.sum(
            head_grad.astype(jnp.float32) * out_rows.astype(jnp.float32), axis=-1, keepdims=True
        )
        prob_grad = contract(head_grad, head_value, 1, 1)
        score_grad = (weights * (prob_grad - row_dots)).astype(jnp.bfloat16)
        query_grad = jnp.dot(score_grad, head_key, preferred_element_type=jnp.float32) * scaling
        key_terms = contract(score_grad, head_query, 0, 0) * scaling
        value_terms = contract(rounded, head_grad, 0, 0)
        out_parts.append(out_rows)
        query_parts.append(query_grad.astype(jnp.bfloat16))
        key_parts.append(key_terms)
        value_parts.append(value_terms)
    return (
        jnp.concatenate(out_parts, axis=1),
        jnp.concatenate(query_parts, axis=1),
        jnp.concatenate(key_parts, axis=1),
        jnp.concatenate(value_parts, axis=1),
    )


def package(tiles_in, pooled_in, devices, spread):
    tiles_here, tile_len, columns = tiles_in.shape
    per_tile = tile_len // POOL
    split_rows = tiles_in.reshape(tiles_here, devices, spread, columns)
    copies = jnp.broadcast_to(
        pooled_in.reshape(tiles_here, 1, per_tile, columns),
        (tiles_here, devices, per_tile, columns),
    )
    return jnp.concatenate([split_rows, copies], axis=2).reshape(
        tiles_here, devices * (spread + per_tile), columns
    )


def listed_shards(query_rows, key_rows, value_rows, out_grad, selected):
    height, columns = query_rows.shape
    devices = lax.axis_size("ctx")
    tiles_here = height // TILE
    spread = TILE // devices
    own_keys = pooled(key_rows)
    own_values = pooled(value_rows)
    key_tiles = key_rows.reshape(tiles_here, TILE, columns)
    value_tiles = value_rows.reshape(tiles_here, TILE, columns)
    joined_keys, joined_values = (
        lax.all_to_all(
            package(key_tiles, own_keys, devices, spread),
            "ctx",
            split_axis=1,
            concat_axis=0,
            tiled=True,
        ),
        lax.all_to_all(
            package(value_tiles, own_values, devices, spread),
            "ctx",
            split_axis=1,
            concat_axis=0,
            tiled=True,
        ),
    )
    held_keys = joined_keys[:, :spread]
    held_values = joined_values[:, :spread]
    pool_keys = joined_keys[:, spread:].reshape(-1, columns)
    pool_values = joined_values[:, spread:].reshape(-1, columns)
    comp_count = pool_keys.shape[0]
    got_keys, got_values = (
        lax.all_to_all(held_keys[selected], "ctx", split_axis=0, concat_axis=2, tiled=True),
        lax.all_to_all(held_values[selected], "ctx", split_axis=0, concat_axis=2, tiled=True),
    )
    fine_keys = got_keys.reshape(tiles_here, SEL * TILE, columns)
    fine_values = got_values.reshape(tiles_here, SEL * TILE, columns)
    out_tiles, query_tiles, key_listed, value_listed = ([], [], [], [])
    keys_all = jnp.concatenate([pool_keys, fine_keys[0]], axis=0)
    values_all = jnp.concatenate([pool_values, fine_values[0]], axis=0)
    out_rows, query_grad, key_terms, value_terms = attend(
        query_rows, out_grad, keys_all, values_all
    )
    out_tiles.append(out_rows)
    query_tiles.append(query_grad)
    coarse_keys = key_terms[:comp_count]
    coarse_values = value_terms[:comp_count]
    key_listed.append(key_terms[comp_count:].astype(jnp.bfloat16))
    value_listed.append(value_terms[comp_count:].astype(jnp.bfloat16))
    own_coarse_keys, own_coarse_values = (
        lax.psum_scatter(coarse_keys, "ctx", scatter_dimension=0, tiled=True),
        lax.psum_scatter(coarse_values, "ctx", scatter_dimension=0, tiled=True),
    )
    listed_keys = jnp.stack(key_listed).reshape(tiles_here * SEL, devices, spread, columns)
    listed_values = jnp.stack(value_listed).reshape(tiles_here * SEL, devices, spread, columns)
    back_keys, back_values = (
        lax.all_to_all(listed_keys, "ctx", split_axis=1, concat_axis=0, tiled=True),
        lax.all_to_all(listed_values, "ctx", split_axis=1, concat_axis=0, tiled=True),
    )
    tile_ids = jnp.arange(selected.shape[0], dtype=jnp.int32)[:, None]
    member = (selected.reshape(1, -1) == tile_ids).astype(jnp.bfloat16)
    entries = member.shape[1]
    sum_keys = jnp.dot(
        member, back_keys.reshape(entries, spread * columns), preferred_element_type=jnp.float32
    )
    sum_values = jnp.dot(
        member, back_values.reshape(entries, spread * columns), preferred_element_type=jnp.float32
    )
    held_key_grad = sum_keys.astype(jnp.bfloat16).reshape(devices, tiles_here, spread, columns)
    held_value_grad = sum_values.astype(jnp.bfloat16).reshape(devices, tiles_here, spread, columns)
    owned_keys, owned_values = (
        lax.all_to_all(held_key_grad, "ctx", split_axis=0, concat_axis=2, tiled=True),
        lax.all_to_all(held_value_grad, "ctx", split_axis=0, concat_axis=2, tiled=True),
    )
    grad_key = (
        owned_keys.reshape(height, columns).astype(jnp.float32)
        + jnp.repeat(own_coarse_keys, POOL, axis=0) / POOL
    ).astype(jnp.bfloat16)
    grad_value = (
        owned_values.reshape(height, columns).astype(jnp.float32)
        + jnp.repeat(own_coarse_values, POOL, axis=0) / POOL
    ).astype(jnp.bfloat16)
    attended = out_tiles[0]
    grad_query = query_tiles[0]
    return (attended, grad_query, grad_key, grad_value, own_coarse_keys, own_coarse_values)


SLOTS = 2


def split_places(devices):
    cores = CORES * PAIR
    levels = devices // cores
    extra = HEADS // levels
    return cores, levels, extra


def owner_of(head):
    cores = CORES * PAIR
    level = head // (cores + 1)
    j = head % (cores + 1)
    spare = j // cores
    extra_at = CORES * (level % PAIR) + CORES - 1
    return level * cores + (1 - spare) * j + spare * extra_at, spare


def holds_two(me):
    cores = CORES * PAIR
    level = me // cores
    return me % cores == CORES * (level % PAIR) + CORES - 1


def meet(devices, me):
    barrier = pltpu.get_barrier_semaphore()
    for k in range(1, devices):
        pl.semaphore_signal(
            barrier,
            inc=1,
            device_id={"ctx": lax.rem(me + k, devices)},
            device_id_type=pl.DeviceIdType.MESH,
        )
    pl.semaphore_wait(barrier, devices - 1)


def spread_kernel(devices, k_ref, v_ref, q_ref, g_ref, rk_ref, rv_ref, rq_ref, rg_ref,
                  send_sem, recv_sem, own_sem):
    me = lax.axis_index("ctx")
    per_level = HEADS // (devices // (CORES * PAIR))
    meet(devices, me)
    two = holds_two(me)
    first = (me // (CORES * PAIR) + 1) * per_level
    rows = pl.ds(pl.multiple_of(me * TILE, TILE), TILE)
    sources = (k_ref, v_ref, q_ref, g_ref)
    targets = (rk_ref, rv_ref, rq_ref, rg_ref)
    for pair in (0, 2):

        def step(i, carry):
            head = lax.rem(first + i, HEADS)
            owner, slot = owner_of(head)
            columns = pl.ds(pl.multiple_of(head * HEAD_DIM, HEAD_DIM), HEAD_DIM)
            for a in (pair, pair + 1):
                src = sources[a].at[:, columns]
                dst = targets[a].at[slot, rows, :]

                @pl.when(owner != me)
                def _():
                    pltpu.make_async_remote_copy(
                        src_ref=src,
                        dst_ref=dst,
                        send_sem=send_sem.at[a],
                        recv_sem=recv_sem.at[a, slot],
                        device_id={"ctx": owner},
                        device_id_type=pl.DeviceIdType.MESH,
                    ).start()

                @pl.when(owner == me)
                def _():
                    pltpu.make_async_copy(src, dst, own_sem.at[a, slot]).start()

            return carry

        lax.fori_loop(0, HEADS, step, 0)
    others = (devices - 1) * TILE

    def wait(slot):
        for a in range(4):
            got = targets[a].at[slot, pl.ds(0, others), :]
            pltpu.make_async_copy(got, got, recv_sem.at[a, slot]).wait()
            own = targets[a].at[slot, rows, :]
            pltpu.make_async_copy(own, own, own_sem.at[a, slot]).wait()

    wait(0)

    @pl.when(two)
    def _():
        wait(1)
        for a in range(4):
            sent = sources[a].at[:, pl.ds(0, (HEADS - 2) * HEAD_DIM)]
            pltpu.make_async_copy(sent, sent, send_sem.at[a]).wait()

    @pl.when(jnp.logical_not(two))
    def _():
        for a in range(4):
            sent = sources[a].at[:, pl.ds(0, (HEADS - 1) * HEAD_DIM)]
            pltpu.make_async_copy(sent, sent, send_sem.at[a]).wait()


def spread(arrays, devices):
    shape = jax.ShapeDtypeStruct((SLOTS, devices * TILE, HEAD_DIM), jnp.bfloat16)
    return pl.pallas_call(
        functools.partial(spread_kernel, devices),
        out_shape=[shape] * 4,
        in_specs=[pl.BlockSpec(memory_space=pl.ANY)] * 4,
        out_specs=[pl.BlockSpec(memory_space=pl.ANY)] * 4,
        scratch_shapes=[
            pltpu.SemaphoreType.DMA((4,)),
            pltpu.SemaphoreType.DMA((4, SLOTS)),
            pltpu.SemaphoreType.DMA((4, SLOTS)),
        ],
        compiler_params=pltpu.CompilerParams(collective_id=0, has_side_effects=True),
        name="spread",
    )(*arrays)


def collect_kernel(devices, o_ref, dq_ref, dk_ref, dv_ref, c_ref,
                   ro_ref, rq_ref, rk_ref, rv_ref, rc_ref, send_sem, recv_sem, own_sem):
    me = lax.axis_index("ctx")
    cores = CORES * PAIR
    meet(devices, me)
    two = holds_two(me)
    level = me // cores
    sources = (o_ref, dq_ref, dk_ref, dv_ref)
    targets = (ro_ref, rq_ref, rk_ref, rv_ref)

    def parts(slot, tile):
        head = level * (cores + 1) + (1 - slot) * (me % cores) + slot * cores
        rows = pl.ds(pl.multiple_of(tile * TILE, TILE), TILE)
        columns = pl.ds(pl.multiple_of(head * HEAD_DIM, HEAD_DIM), HEAD_DIM)
        for a in range(4):
            yield a, sources[a].at[slot, rows, :], targets[a].at[:, columns]
        yield 4, c_ref.at[slot, tile], rc_ref.at[head]

    def send(slot):
        def step(i, carry):
            tile = lax.rem(me + 1 + i, devices)
            for a, src, dst in parts(slot, tile):
                pltpu.make_async_remote_copy(
                    src_ref=src,
                    dst_ref=dst,
                    send_sem=send_sem.at[a, slot],
                    recv_sem=recv_sem.at[a],
                    device_id={"ctx": tile},
                    device_id_type=pl.DeviceIdType.MESH,
                ).start()
            return carry

        lax.fori_loop(0, devices - 1, step, 0)
        for a, src, dst in parts(slot, me):
            pltpu.make_async_copy(src, dst, own_sem.at[a, slot]).start()

    def sent(slot):
        for a, src, dst in parts(slot, me):
            pltpu.make_async_copy(src, dst, own_sem.at[a, slot]).wait()
        for a in range(4):
            gone = sources[a].at[slot, pl.ds(0, (devices - 1) * TILE), :]
            pltpu.make_async_copy(gone, gone, send_sem.at[a, slot]).wait()
        gone = c_ref.at[slot, pl.ds(0, devices - 1)]
        pltpu.make_async_copy(gone, gone, send_sem.at[4, slot]).wait()

    def got(heads):
        for a in range(4):
            here = targets[a].at[:, pl.ds(0, heads * HEAD_DIM)]
            pltpu.make_async_copy(here, here, recv_sem.at[a]).wait()
        here = rc_ref.at[pl.ds(0, heads)]
        pltpu.make_async_copy(here, here, recv_sem.at[4]).wait()

    send(0)

    @pl.when(two)
    def _():
        send(1)
        sent(1)
        got(HEADS - 2)

    @pl.when(jnp.logical_not(two))
    def _():
        got(HEADS - 1)

    sent(0)


def collect(arrays, devices):
    flat = jax.ShapeDtypeStruct((TILE, HEADS * HEAD_DIM), jnp.bfloat16)
    coarse = jax.ShapeDtypeStruct((HEADS, 8, HEAD_DIM), jnp.float32)
    return pl.pallas_call(
        functools.partial(collect_kernel, devices),
        out_shape=[flat] * 4 + [coarse],
        in_specs=[pl.BlockSpec(memory_space=pl.ANY)] * 5,
        out_specs=[pl.BlockSpec(memory_space=pl.ANY)] * 5,
        scratch_shapes=[
            pltpu.SemaphoreType.DMA((5, SLOTS)),
            pltpu.SemaphoreType.DMA((5,)),
            pltpu.SemaphoreType.DMA((5, SLOTS)),
        ],
        compiler_params=pltpu.CompilerParams(collective_id=1, has_side_effects=True),
        name="collect",
    )(*arrays)


def whole_head_kernel(place_ref, count_ref, k_ref, v_ref, q_ref, g_ref,
                      o_ref, dq_ref, dk_ref, dv_ref, c_ref, joined, keys_t, values_t, total):
    tokens = k_ref.shape[0]
    tiles = tokens // TILE
    pools = tokens // POOL
    scaling = HEAD_DIM ** (-0.5)
    rate = scaling * math.log2(math.e)

    @pl.when(pl.program_id(0) < count_ref[0])
    def _():
        for ref, at, turned in ((k_ref, 0, keys_t), (v_ref, HEAD_DIM, values_t)):
            rows = ref[...]
            wide = rows.astype(jnp.float32)
            means = jnp.sum(wide.reshape(pools, POOL, HEAD_DIM), axis=1) * (1.0 / POOL)
            means = means.astype(jnp.bfloat16)
            joined[:tokens, at : at + HEAD_DIM] = rows
            joined[tokens:, at : at + HEAD_DIM] = means
            turned[:, :tokens] = rows.T
            turned[:, tokens:] = means.T
        total[...] = jnp.zeros_like(total)

        def tile_step(t, carry):
            rows = pl.ds(pl.multiple_of(t * TILE, TILE), TILE)
            query = q_ref[rows, :]
            grad = g_ref[rows, :]
            blank = jnp.zeros_like(query)
            paired = jnp.concatenate(
                [
                    jnp.concatenate([query, blank], axis=1),
                    jnp.concatenate([blank, grad], axis=1),
                ],
                axis=0,
            )
            starts = [pl.multiple_of(place_ref[t * SEL + j] * TILE, TILE) for j in range(SEL)]
            listed = jnp.concatenate(
                [joined[pl.ds(s, TILE), :] for s in starts] + [joined[tokens:, :]], axis=0
            )
            both = contract(listed, paired, 1, 1)
            scores = both[:, :TILE]
            prob_grad = both[:, TILE:]
            summit = jnp.max(scores, axis=0, keepdims=True)
            raised = jnp.exp2((scores - summit) * rate)
            scale = 1.0 / jnp.sum(raised, axis=0, keepdims=True)
            dots = jnp.sum(raised * prob_grad, axis=0, keepdims=True) * scale
            weights = raised * scale
            score_grad = (weights * (prob_grad - dots)).astype(jnp.bfloat16)
            rounded = weights.astype(jnp.bfloat16)
            listed_kt = jnp.concatenate(
                [keys_t[:, pl.ds(s, TILE)] for s in starts] + [keys_t[:, tokens:]], axis=1
            )
            listed_vt = jnp.concatenate(
                [values_t[:, pl.ds(s, TILE)] for s in starts] + [values_t[:, tokens:]], axis=1
            )
            out_t = jnp.dot(listed_vt, rounded, preferred_element_type=jnp.float32)
            dq_t = jnp.dot(listed_kt, score_grad, preferred_element_type=jnp.float32) * scaling
            o_ref[rows, :] = out_t.T.astype(jnp.bfloat16)
            dq_ref[rows, :] = dq_t.T.astype(jnp.bfloat16)
            terms = jnp.dot(
                jnp.concatenate([score_grad, rounded], axis=1),
                paired,
                preferred_element_type=jnp.float32,
            )
            for j, s in enumerate(starts):
                total[pl.ds(s, TILE), :] += terms[j * TILE : (j + 1) * TILE]
            total[tokens:, :] += terms[SEL * TILE :]
            return carry

        lax.fori_loop(0, tiles, tile_step, 0)
        per_tile = TILE // POOL
        for ref, at, factor in ((dk_ref, 0, scaling), (dv_ref, HEAD_DIM, 1.0)):
            coarse = total[tokens:, at : at + HEAD_DIM] * factor
            fine = total[:tokens, at : at + HEAD_DIM] * factor
            fine = fine.reshape(pools, POOL, HEAD_DIM) + (coarse * (1.0 / POOL))[:, None, :]
            ref[...] = fine.reshape(tokens, HEAD_DIM).astype(jnp.bfloat16)
            start = 0 if at == 0 else per_tile
            for tile in range(tiles):
                c_ref[tile, start : start + per_tile, :] = coarse[
                    tile * per_tile : (tile + 1) * per_tile
                ]


def whole_heads(place, count, rk, rv, rq, rg):
    tokens = rk.shape[1]
    tiles = tokens // TILE
    pools = tokens // POOL
    used = lambda s, place, count: (jnp.minimum(s, count[0] - 1), 0, 0)
    here = lambda s, place, count: (s, 0, 0)
    rows = jax.ShapeDtypeStruct((SLOTS, tokens, HEAD_DIM), jnp.bfloat16)
    block = (None, tokens, HEAD_DIM)
    return pl.pallas_call(
        whole_head_kernel,
        grid_spec=pltpu.PrefetchScalarGridSpec(
            num_scalar_prefetch=2,
            grid=(SLOTS,),
            in_specs=[pl.BlockSpec(block, used)] * 4,
            out_specs=[pl.BlockSpec(block, here)] * 4
            + [pl.BlockSpec((None, tiles, 8, HEAD_DIM), lambda s, place, count: (s, 0, 0, 0))],
            scratch_shapes=[
                pltpu.VMEM((tokens + pools, 2 * HEAD_DIM), jnp.bfloat16),
                pltpu.VMEM((HEAD_DIM, tokens + pools), jnp.bfloat16),
                pltpu.VMEM((HEAD_DIM, tokens + pools), jnp.bfloat16),
                pltpu.VMEM((tokens + pools, 2 * HEAD_DIM), jnp.float32),
            ],
        ),
        out_shape=[rows] * 4
        + [jax.ShapeDtypeStruct((SLOTS, tiles, 8, HEAD_DIM), jnp.float32)],
        name="whole_heads",
    )(place, count, rk, rv, rq, rg)


def exchange_shards(query_rows, key_rows, value_rows, out_grad, selected):
    devices = lax.axis_size("ctx")
    me = lax.axis_index("ctx")
    rk, rv, rq, rg = spread((key_rows, value_rows, query_rows, out_grad), devices)
    count = jnp.where(holds_two(me), 2, 1).astype(jnp.int32).reshape(1)
    out, dq, dk, dv, coarse = whole_heads(selected.reshape(-1), count, rk, rv, rq, rg)
    out, dq, dk, dv, coarse = collect((out, dq, dk, dv, coarse), devices)
    per_tile = TILE // POOL
    flat = lambda part: part.transpose(1, 0, 2).reshape(per_tile, HEADS * HEAD_DIM)
    return (
        out,
        dq,
        dk,
        dv,
        flat(coarse[:, :per_tile]),
        flat(coarse[:, per_tile : 2 * per_tile]),
    )


def shards(query_rows, key_rows, value_rows, out_grad, selected):
    devices = lax.axis_size("ctx")
    fits = devices == 4 * CORES * PAIR and query_rows.shape[0] == TILE
    chosen = exchange_shards if fits else listed_shards
    return chosen(query_rows, key_rows, value_rows, out_grad, selected)


def solution(mesh):
    in_specs = (
        P(("groups", "ctx"), None),
        P(("groups", "ctx"), None),
        P(("groups", "ctx"), None),
        P(("groups", "ctx"), None),
        P("groups", None),
    )
    out_specs = (
        P(("groups", "ctx"), None),
        P(("groups", "ctx"), None),
        P(("groups", "ctx"), None),
        P(("groups", "ctx"), None),
        P(("groups", "ctx"), None),
        P(("groups", "ctx"), None),
    )
    return jax.shard_map(shards, mesh=mesh, in_specs=in_specs, out_specs=out_specs, check_vma=False)
```

```python
import functools
import math

import jax
import jax.numpy as jnp
from jax import lax
from jax.experimental import pallas as pl
from jax.experimental.pallas import tpu as pltpu
from jax.sharding import PartitionSpec as P

HEADS = 20
HEAD_DIM = 128
TILE = 128
POOL = 64
SEL = 8
CORES = 2
PAIR = 2


def pooled(rows):
    return jnp.mean(rows.astype(jnp.float32).reshape(-1, POOL, rows.shape[1]), axis=1).astype(
        jnp.bfloat16
    )


def contract(left, right, left_dim, right_dim):
    return lax.dot_general(
        left, right, (((left_dim,), (right_dim,)), ((), ())), preferred_element_type=jnp.float32
    )


def attend(queries, grads_out, keys_all, values_all):
    scaling = HEAD_DIM ** (-0.5)
    out_parts, query_parts, key_parts, value_parts = ([], [], [], [])
    for head in range(HEADS):
        lower = head * HEAD_DIM
        upper = lower + HEAD_DIM
        head_query = queries[:, lower:upper]
        head_grad = grads_out[:, lower:upper]
        head_key = keys_all[:, lower:upper]
        head_value = values_all[:, lower:upper]
        scores = contract(head_query, head_key, 1, 1) * scaling
        summit = jnp.max(scores, axis=-1, keepdims=True)
        raised = jnp.exp(scores - summit)
        weights = raised / jnp.sum(raised, axis=-1, keepdims=True)
        rounded = weights.astype(jnp.bfloat16)
        out_rows = jnp.dot(rounded, head_value, preferred_element_type=jnp.float32).astype(
            jnp.bfloat16
        )
        row_dots = jnp.sum(
            head_grad.astype(jnp.float32) * out_rows.astype(jnp.float32), axis=-1, keepdims=True
        )
        prob_grad = contract(head_grad, head_value, 1, 1)
        score_grad = (weights * (prob_grad - row_dots)).astype(jnp.bfloat16)
        query_grad = jnp.dot(score_grad, head_key, preferred_element_type=jnp.float32) * scaling
        key_terms = contract(score_grad, head_query, 0, 0) * scaling
        value_terms = contract(rounded, head_grad, 0, 0)
        out_parts.append(out_rows)
        query_parts.append(query_grad.astype(jnp.bfloat16))
        key_parts.append(key_terms)
        value_parts.append(value_terms)
    return (
        jnp.concatenate(out_parts, axis=1),
        jnp.concatenate(query_parts, axis=1),
        jnp.concatenate(key_parts, axis=1),
        jnp.concatenate(value_parts, axis=1),
    )


def package(tiles_in, pooled_in, devices, spread):
    tiles_here, tile_len, columns = tiles_in.shape
    per_tile = tile_len // POOL
    split_rows = tiles_in.reshape(tiles_here, devices, spread, columns)
    copies = jnp.broadcast_to(
        pooled_in.reshape(tiles_here, 1, per_tile, columns),
        (tiles_here, devices, per_tile, columns),
    )
    return jnp.concatenate([split_rows, copies], axis=2).reshape(
        tiles_here, devices * (spread + per_tile), columns
    )


def listed_shards(query_rows, key_rows, value_rows, out_grad, selected):
    height, columns = query_rows.shape
    devices = lax.axis_size("ctx")
    tiles_here = height // TILE
    spread = TILE // devices
    own_keys = pooled(key_rows)
    own_values = pooled(value_rows)
    key_tiles = key_rows.reshape(tiles_here, TILE, columns)
    value_tiles = value_rows.reshape(tiles_here, TILE, columns)
    joined_keys, joined_values = (
        lax.all_to_all(
            package(key_tiles, own_keys, devices, spread),
            "ctx",
            split_axis=1,
            concat_axis=0,
            tiled=True,
        ),
        lax.all_to_all(
            package(value_tiles, own_values, devices, spread),
            "ctx",
            split_axis=1,
            concat_axis=0,
            tiled=True,
        ),
    )
    held_keys = joined_keys[:, :spread]
    held_values = joined_values[:, :spread]
    pool_keys = joined_keys[:, spread:].reshape(-1, columns)
    pool_values = joined_values[:, spread:].reshape(-1, columns)
    comp_count = pool_keys.shape[0]
    got_keys, got_values = (
        lax.all_to_all(held_keys[selected], "ctx", split_axis=0, concat_axis=2, tiled=True),
        lax.all_to_all(held_values[selected], "ctx", split_axis=0, concat_axis=2, tiled=True),
    )
    fine_keys = got_keys.reshape(tiles_here, SEL * TILE, columns)
    fine_values = got_values.reshape(tiles_here, SEL * TILE, columns)
    out_tiles, query_tiles, key_listed, value_listed = ([], [], [], [])
    keys_all = jnp.concatenate([pool_keys, fine_keys[0]], axis=0)
    values_all = jnp.concatenate([pool_values, fine_values[0]], axis=0)
    out_rows, query_grad, key_terms, value_terms = attend(
        query_rows, out_grad, keys_all, values_all
    )
    out_tiles.append(out_rows)
    query_tiles.append(query_grad)
    coarse_keys = key_terms[:comp_count]
    coarse_values = value_terms[:comp_count]
    key_listed.append(key_terms[comp_count:].astype(jnp.bfloat16))
    value_listed.append(value_terms[comp_count:].astype(jnp.bfloat16))
    own_coarse_keys, own_coarse_values = (
        lax.psum_scatter(coarse_keys, "ctx", scatter_dimension=0, tiled=True),
        lax.psum_scatter(coarse_values, "ctx", scatter_dimension=0, tiled=True),
    )
    listed_keys = jnp.stack(key_listed).reshape(tiles_here * SEL, devices, spread, columns)
    listed_values = jnp.stack(value_listed).reshape(tiles_here * SEL, devices, spread, columns)
    back_keys, back_values = (
        lax.all_to_all(listed_keys, "ctx", split_axis=1, concat_axis=0, tiled=True),
        lax.all_to_all(listed_values, "ctx", split_axis=1, concat_axis=0, tiled=True),
    )
    tile_ids = jnp.arange(selected.shape[0], dtype=jnp.int32)[:, None]
    member = (selected.reshape(1, -1) == tile_ids).astype(jnp.bfloat16)
    entries = member.shape[1]
    sum_keys = jnp.dot(
        member, back_keys.reshape(entries, spread * columns), preferred_element_type=jnp.float32
    )
    sum_values = jnp.dot(
        member, back_values.reshape(entries, spread * columns), preferred_element_type=jnp.float32
    )
    held_key_grad = sum_keys.astype(jnp.bfloat16).reshape(devices, tiles_here, spread, columns)
    held_value_grad = sum_values.astype(jnp.bfloat16).reshape(devices, tiles_here, spread, columns)
    owned_keys, owned_values = (
        lax.all_to_all(held_key_grad, "ctx", split_axis=0, concat_axis=2, tiled=True),
        lax.all_to_all(held_value_grad, "ctx", split_axis=0, concat_axis=2, tiled=True),
    )
    grad_key = (
        owned_keys.reshape(height, columns).astype(jnp.float32)
        + jnp.repeat(own_coarse_keys, POOL, axis=0) / POOL
    ).astype(jnp.bfloat16)
    grad_value = (
        owned_values.reshape(height, columns).astype(jnp.float32)
        + jnp.repeat(own_coarse_values, POOL, axis=0) / POOL
    ).astype(jnp.bfloat16)
    attended = out_tiles[0]
    grad_query = query_tiles[0]
    return (attended, grad_query, grad_key, grad_value, own_coarse_keys, own_coarse_values)


SLOTS = 2
CORES_HERE = CORES * PAIR


def remote(src, dst, sent, got, target):
    return pltpu.make_async_remote_copy(
        src_ref=src,
        dst_ref=dst,
        send_sem=sent,
        recv_sem=got,
        device_id={"ctx": target},
        device_id_type=pl.DeviceIdType.MESH,
    )


def wait_for(ref, semaphore):
    pltpu.make_async_copy(ref, ref, semaphore).wait()


def block(index, size):
    return pl.ds(pl.multiple_of(index * size, size), size)


def meet(devices, me):
    barrier = pltpu.get_barrier_semaphore()
    for k in range(1, devices):
        pl.semaphore_signal(
            barrier,
            inc=1,
            device_id={"ctx": lax.rem(me + k, devices)},
            device_id_type=pl.DeviceIdType.MESH,
        )
    pl.semaphore_wait(barrier, devices - 1)


def fused_kernel(devices, place_ref, spot, k_ref, v_ref, q_ref, g_ref,
                 ro_ref, rq_ref, rk_ref, rv_ref, rc_ref,
                 keys_in, values_in, queries, grads, out_o, out_q, out_k, out_v, out_c,
                 joined, joined_pool, keys_t, keys_pool, values_t, values_pool, pairs, kept,
                 kept_pool, total,
                 send_in, kv_sem, own_sem, q_sem, g_sem, send_out, back_sem, own_out):
    me = lax.axis_index("ctx")
    levels = devices // CORES_HERE
    per_level = HEADS // levels
    tokens = devices * TILE
    pools = tokens // POOL
    per_tile = TILE // POOL
    listed_rows = SEL * TILE
    level = me // CORES_HERE
    upper = level // 2
    near = (1 - upper) * level + upper * (levels - 1 - level)
    extra_at = CORES * (level % PAIR) + CORES - 1
    two = me % CORES_HERE == extra_at
    apart = me % CORES_HERE - extra_at
    count = 1 + (CORES_HERE * CORES_HERE - apart * apart) // (CORES_HERE * CORES_HERE)
    scaling = HEAD_DIM ** (-0.5)
    rate = scaling * math.log2(math.e)

    def level_at(step):
        turn = step + near * (1 - step // 2) * (1 - 2 * step)
        return (1 - upper) * turn + upper * (levels - 1 - turn)

    meet(devices, me)

    my_rows = block(me, TILE)

    def send_pair(index):
        def step(i, carry):
            goal = level_at(i // per_level)
            j = lax.rem(i + me, per_level)
            spare = j // CORES_HERE
            owner = (
                goal * CORES_HERE
                + (1 - spare) * j
                + spare * (CORES * (goal % PAIR) + CORES - 1)
            )
            columns = block(goal * per_level + j, HEAD_DIM)
            if index == 0:
                moves = [
                    (k_ref, keys_in.at[spare, my_rows, :], kv_sem.at[0, spare]),
                    (v_ref, values_in.at[spare, my_rows, :], kv_sem.at[1, spare]),
                ]
            else:
                moves = [
                    (q_ref, queries.at[spare, my_rows, :], q_sem.at[spare, me]),
                    (g_ref, grads.at[spare, my_rows, :], g_sem.at[spare, me]),
                ]

            @pl.when(owner != me)
            def _():
                for n, (src, dst, got) in enumerate(moves):
                    remote(src.at[:, columns], dst, send_in.at[2 * index + n], got, owner).start()

            @pl.when(owner == me)
            def _():
                for n, (src, dst, got) in enumerate(moves):
                    arrived = own_sem.at[n, spare] if index == 0 else got
                    pltpu.make_async_copy(src.at[:, columns], dst, arrived).start()

            return carry

        lax.fori_loop(0, HEADS, step, 0)

    send_pair(0)
    send_pair(1)

    for i in range(CORES_HERE):
        kept[i, SEL] = jnp.zeros((TILE, 2 * HEAD_DIM), jnp.bfloat16)
    out_c[...] = jnp.zeros_like(out_c)

    def send_back(slot, tile, moves):
        @pl.when(tile != me)
        def _():
            for a, src, dst in moves:
                remote(src, dst, send_out.at[a, slot], back_sem.at[a], tile).start()

        @pl.when(tile == me)
        def _():
            for a, src, dst in moves:
                pltpu.make_async_copy(src, dst, own_out.at[a, slot]).start()

    def run_head(slot, carry):
        head = level * per_level + (1 - slot) * (me % CORES_HERE) + slot * CORES_HERE
        columns = block(head, HEAD_DIM)

        def send_rows(tile):
            rows = block(tile, TILE)
            send_back(
                slot,
                tile,
                [
                    (0, out_o.at[slot, rows, :], ro_ref.at[:, columns]),
                    (1, out_q.at[slot, rows, :], rq_ref.at[:, columns]),
                ],
            )

        for n, (source, turned, turned_pool) in enumerate(
            ((keys_in, keys_t, keys_pool), (values_in, values_t, values_pool))
        ):
            wait_for(source.at[slot, pl.ds(0, tokens - TILE), :], kv_sem.at[n, slot])
            wait_for(source.at[slot, my_rows, :], own_sem.at[n, slot])
            part = slice(n * HEAD_DIM, (n + 1) * HEAD_DIM)
            rows = source[slot]
            means = jnp.sum(rows.astype(jnp.float32).reshape(pools, POOL, HEAD_DIM), axis=1)
            means = (means * (1.0 / POOL)).astype(jnp.bfloat16)
            joined_pool[:, part] = means
            turned_pool[...] = means.T
            for tile in range(devices):
                one = rows[tile * TILE : (tile + 1) * TILE]
                joined[tile, :, part] = one
                turned[tile] = one.T
        total[...] = jnp.zeros_like(total)

        def tile_step(n, carry):
            i = lax.rem(n, CORES_HERE)
            t = level_at(n // CORES_HERE) * CORES_HERE + i
            rows = block(t, TILE)

            @pl.when(n > 0)
            def _():
                before = n - 1
                send_rows(
                    level_at(before // CORES_HERE) * CORES_HERE + lax.rem(before, CORES_HERE)
                )

            wait_for(queries.at[slot, rows, :], q_sem.at[slot, t])
            wait_for(grads.at[slot, rows, :], g_sem.at[slot, t])
            query = queries[slot, rows, :]
            grad = grads[slot, rows, :]
            blank = jnp.zeros_like(query)
            paired = jnp.concatenate(
                [
                    jnp.concatenate([query, blank], axis=1),
                    jnp.concatenate([blank, grad], axis=1),
                ],
                axis=0,
            )
            pairs[i] = paired
            places = [place_ref[t, j] for j in range(SEL)]
            listed = jnp.concatenate(
                [joined[place] for place in places] + [joined_pool[...]], axis=0
            )
            both = contract(listed, paired, 1, 1)
            scores = both[:, :TILE]
            prob_grad = both[:, TILE:]
            summit = jnp.max(scores, axis=0, keepdims=True)
            raised = jnp.exp2((scores - summit) * rate)
            scale = 1.0 / jnp.sum(raised, axis=0, keepdims=True)
            dots = jnp.sum(raised * prob_grad, axis=0, keepdims=True) * scale
            weights = raised * scale
            score_grad = (weights * (prob_grad - dots)).astype(jnp.bfloat16)
            rounded = weights.astype(jnp.bfloat16)
            for part, values in ((0, score_grad), (HEAD_DIM, rounded)):
                for j in range(SEL):
                    kept[i, j, :, part : part + HEAD_DIM] = values[j * TILE : (j + 1) * TILE]
                kept_pool[i, :, part : part + HEAD_DIM] = values[listed_rows:]
            listed_kt = jnp.concatenate(
                [keys_t[place] for place in places] + [keys_pool[...]], axis=1
            )
            listed_vt = jnp.concatenate(
                [values_t[place] for place in places] + [values_pool[...]], axis=1
            )
            out_t = jnp.dot(listed_vt, rounded, preferred_element_type=jnp.float32)
            dq_t = jnp.dot(listed_kt, score_grad, preferred_element_type=jnp.float32) * scaling
            out_o[slot, rows, :] = out_t.T.astype(jnp.bfloat16)
            out_q[slot, rows, :] = dq_t.T.astype(jnp.bfloat16)
            return carry

        def add_terms(g, carry):
            first = level_at(g) * CORES_HERE
            facing = pairs[...].reshape(CORES_HERE * 2 * TILE, 2 * HEAD_DIM)
            for u in range(devices):
                found = jnp.concatenate(
                    [kept[i, spot[first + i, u]] for i in range(CORES_HERE)],
                    axis=1,
                )
                total[u * TILE : (u + 1) * TILE, :] += jnp.dot(
                    found, facing, preferred_element_type=jnp.float32
                )
            found = jnp.concatenate([kept_pool[i] for i in range(CORES_HERE)], axis=1)
            total[tokens:, :] += jnp.dot(found, facing, preferred_element_type=jnp.float32)
            return carry

        def group_step(g, carry):
            lax.fori_loop(g * CORES_HERE, (g + 1) * CORES_HERE, tile_step, 0)
            return add_terms(g, carry)

        lax.fori_loop(0, levels, group_step, 0)
        send_rows(level_at(levels - 1) * CORES_HERE + CORES_HERE - 1)
        for ref, at, factor in ((out_k, 0, scaling), (out_v, HEAD_DIM, 1.0)):
            coarse = total[tokens:, at : at + HEAD_DIM] * factor
            fine = total[:tokens, at : at + HEAD_DIM] * factor
            fine = fine.reshape(pools, POOL, HEAD_DIM) + (coarse * (1.0 / POOL))[:, None, :]
            ref[slot] = fine.reshape(tokens, HEAD_DIM).astype(jnp.bfloat16)
            start = 0 if at == 0 else per_tile
            for tile in range(devices):
                out_c[slot, tile, start : start + per_tile, :] = coarse[
                    tile * per_tile : (tile + 1) * per_tile
                ]

        def send_sums(n, carry):
            tile = level_at(n // CORES_HERE) * CORES_HERE + lax.rem(n, CORES_HERE)
            rows = block(tile, TILE)
            send_back(
                slot,
                tile,
                [
                    (2, out_k.at[slot, rows, :], rk_ref.at[:, columns]),
                    (3, out_v.at[slot, rows, :], rv_ref.at[:, columns]),
                    (4, out_c.at[slot, tile], rc_ref.at[head]),
                ],
            )
            return carry

        lax.fori_loop(0, devices, send_sums, 0)
        return carry

    lax.fori_loop(0, count, run_head, 0)

    stores = (out_o, out_q, out_k, out_v)
    landed = (ro_ref, rq_ref, rk_ref, rv_ref)

    def sent(slot):
        for a, ref in enumerate(stores):
            wait_for(ref.at[slot, pl.ds(0, tokens - TILE), :], send_out.at[a, slot])
            wait_for(ref.at[slot, my_rows, :], own_out.at[a, slot])
        wait_for(out_c.at[slot, pl.ds(0, devices - 1)], send_out.at[4, slot])
        wait_for(out_c.at[slot, me], own_out.at[4, slot])

    def finish(own):
        for n, ref in enumerate((k_ref, v_ref, q_ref, g_ref)):
            wait_for(ref.at[:, pl.ds(0, (HEADS - own) * HEAD_DIM)], send_in.at[n])
        for a, ref in enumerate(landed):
            wait_for(ref.at[:, pl.ds(0, (HEADS - own) * HEAD_DIM)], back_sem.at[a])
        wait_for(rc_ref.at[pl.ds(0, HEADS - own)], back_sem.at[4])

    sent(0)

    @pl.when(two)
    def _():
        sent(1)
        finish(2)

    @pl.when(jnp.logical_not(two))
    def _():
        finish(1)


def spots(selected):
    listed = selected[:, :, None] == jnp.arange(selected.shape[0], dtype=jnp.int32)
    shift = jnp.arange(SEL, dtype=jnp.int32)[None, :, None] - SEL
    return SEL + jnp.sum(jnp.where(listed, shift, 0), axis=1, dtype=jnp.int32)


def fused(selected, arrays, devices):
    tokens = devices * TILE
    pools = tokens // POOL
    flat = jax.ShapeDtypeStruct((TILE, HEADS * HEAD_DIM), jnp.bfloat16)
    coarse = jax.ShapeDtypeStruct((HEADS, 8, HEAD_DIM), jnp.float32)
    slabs = pltpu.VMEM((SLOTS, tokens, HEAD_DIM), jnp.bfloat16)
    turned = pltpu.VMEM((devices, HEAD_DIM, TILE), jnp.bfloat16)
    turned_pool = pltpu.VMEM((HEAD_DIM, pools), jnp.bfloat16)
    return pl.pallas_call(
        functools.partial(fused_kernel, devices),
        out_shape=[flat] * 4 + [coarse],
        in_specs=[pl.BlockSpec(memory_space=pltpu.SMEM)] * 2 + [pl.BlockSpec(memory_space=pl.ANY)] * 4,
        out_specs=[pl.BlockSpec(memory_space=pl.ANY)] * 5,
        scratch_shapes=[
            slabs,
            slabs,
            slabs,
            slabs,
            slabs,
            slabs,
            slabs,
            slabs,
            pltpu.VMEM((SLOTS, devices, 8, HEAD_DIM), jnp.float32),
            pltpu.VMEM((devices, TILE, 2 * HEAD_DIM), jnp.bfloat16),
            pltpu.VMEM((pools, 2 * HEAD_DIM), jnp.bfloat16),
            turned,
            turned_pool,
            turned,
            turned_pool,
            pltpu.VMEM((CORES_HERE, 2 * TILE, 2 * HEAD_DIM), jnp.bfloat16),
            pltpu.VMEM((CORES_HERE, SEL + 1, TILE, 2 * HEAD_DIM), jnp.bfloat16),
            pltpu.VMEM((CORES_HERE, pools, 2 * HEAD_DIM), jnp.bfloat16),
            pltpu.VMEM((tokens + pools, 2 * HEAD_DIM), jnp.float32),
            pltpu.SemaphoreType.DMA((4,)),
            pltpu.SemaphoreType.DMA((2, SLOTS)),
            pltpu.SemaphoreType.DMA((2, SLOTS)),
            pltpu.SemaphoreType.DMA((SLOTS, devices)),
            pltpu.SemaphoreType.DMA((SLOTS, devices)),
            pltpu.SemaphoreType.DMA((5, SLOTS)),
            pltpu.SemaphoreType.DMA((5,)),
            pltpu.SemaphoreType.DMA((5, SLOTS)),
        ],
        compiler_params=pltpu.CompilerParams(collective_id=0, has_side_effects=True),
        name="exchange_heads",
    )(selected, spots(selected), *arrays)


def exchange_shards(query_rows, key_rows, value_rows, out_grad, selected):
    devices = lax.axis_size("ctx")
    out, dq, dk, dv, coarse = fused(
        selected, (key_rows, value_rows, query_rows, out_grad), devices
    )
    per_tile = TILE // POOL
    flat = lambda part: part.transpose(1, 0, 2).reshape(per_tile, HEADS * HEAD_DIM)
    return (
        out,
        dq,
        dk,
        dv,
        flat(coarse[:, :per_tile]),
        flat(coarse[:, per_tile : 2 * per_tile]),
    )


def shards(query_rows, key_rows, value_rows, out_grad, selected):
    devices = lax.axis_size("ctx")
    fits = devices == 4 * CORES * PAIR and query_rows.shape[0] == TILE
    chosen = exchange_shards if fits else listed_shards
    return chosen(query_rows, key_rows, value_rows, out_grad, selected)


def solution(mesh):
    in_specs = (
        P(("groups", "ctx"), None),
        P(("groups", "ctx"), None),
        P(("groups", "ctx"), None),
        P(("groups", "ctx"), None),
        P("groups", None),
    )
    out_specs = (
        P(("groups", "ctx"), None),
        P(("groups", "ctx"), None),
        P(("groups", "ctx"), None),
        P(("groups", "ctx"), None),
        P(("groups", "ctx"), None),
        P(("groups", "ctx"), None),
    )
    return jax.shard_map(shards, mesh=mesh, in_specs=in_specs, out_specs=out_specs, check_vma=False)
```

```python
import functools
import math

import jax
import jax.numpy as jnp
from jax import lax
from jax.experimental import pallas as pl
from jax.experimental.pallas import tpu as pltpu
from jax.sharding import PartitionSpec as P

HEADS = 20
HEAD_DIM = 128
TILE = 128
POOL = 64
SEL = 8
CORES = 2
PAIR = 2


def pooled(rows):
    return jnp.mean(rows.astype(jnp.float32).reshape(-1, POOL, rows.shape[1]), axis=1).astype(
        jnp.bfloat16
    )


def contract(left, right, left_dim, right_dim):
    return lax.dot_general(
        left, right, (((left_dim,), (right_dim,)), ((), ())), preferred_element_type=jnp.float32
    )


def attend(queries, grads_out, keys_all, values_all):
    scaling = HEAD_DIM ** (-0.5)
    out_parts, query_parts, key_parts, value_parts = ([], [], [], [])
    for head in range(HEADS):
        lower = head * HEAD_DIM
        upper = lower + HEAD_DIM
        head_query = queries[:, lower:upper]
        head_grad = grads_out[:, lower:upper]
        head_key = keys_all[:, lower:upper]
        head_value = values_all[:, lower:upper]
        scores = contract(head_query, head_key, 1, 1) * scaling
        summit = jnp.max(scores, axis=-1, keepdims=True)
        raised = jnp.exp(scores - summit)
        weights = raised / jnp.sum(raised, axis=-1, keepdims=True)
        rounded = weights.astype(jnp.bfloat16)
        out_rows = jnp.dot(rounded, head_value, preferred_element_type=jnp.float32).astype(
            jnp.bfloat16
        )
        row_dots = jnp.sum(
            head_grad.astype(jnp.float32) * out_rows.astype(jnp.float32), axis=-1, keepdims=True
        )
        prob_grad = contract(head_grad, head_value, 1, 1)
        score_grad = (weights * (prob_grad - row_dots)).astype(jnp.bfloat16)
        query_grad = jnp.dot(score_grad, head_key, preferred_element_type=jnp.float32) * scaling
        key_terms = contract(score_grad, head_query, 0, 0) * scaling
        value_terms = contract(rounded, head_grad, 0, 0)
        out_parts.append(out_rows)
        query_parts.append(query_grad.astype(jnp.bfloat16))
        key_parts.append(key_terms)
        value_parts.append(value_terms)
    return (
        jnp.concatenate(out_parts, axis=1),
        jnp.concatenate(query_parts, axis=1),
        jnp.concatenate(key_parts, axis=1),
        jnp.concatenate(value_parts, axis=1),
    )


def package(tiles_in, pooled_in, devices, spread):
    tiles_here, tile_len, columns = tiles_in.shape
    per_tile = tile_len // POOL
    split_rows = tiles_in.reshape(tiles_here, devices, spread, columns)
    copies = jnp.broadcast_to(
        pooled_in.reshape(tiles_here, 1, per_tile, columns),
        (tiles_here, devices, per_tile, columns),
    )
    return jnp.concatenate([split_rows, copies], axis=2).reshape(
        tiles_here, devices * (spread + per_tile), columns
    )


def listed_shards(query_rows, key_rows, value_rows, out_grad, selected):
    height, columns = query_rows.shape
    devices = lax.axis_size("ctx")
    tiles_here = height // TILE
    spread = TILE // devices
    own_keys = pooled(key_rows)
    own_values = pooled(value_rows)
    key_tiles = key_rows.reshape(tiles_here, TILE, columns)
    value_tiles = value_rows.reshape(tiles_here, TILE, columns)
    joined_keys, joined_values = (
        lax.all_to_all(
            package(key_tiles, own_keys, devices, spread),
            "ctx",
            split_axis=1,
            concat_axis=0,
            tiled=True,
        ),
        lax.all_to_all(
            package(value_tiles, own_values, devices, spread),
            "ctx",
            split_axis=1,
            concat_axis=0,
            tiled=True,
        ),
    )
    held_keys = joined_keys[:, :spread]
    held_values = joined_values[:, :spread]
    pool_keys = joined_keys[:, spread:].reshape(-1, columns)
    pool_values = joined_values[:, spread:].reshape(-1, columns)
    comp_count = pool_keys.shape[0]
    got_keys, got_values = (
        lax.all_to_all(held_keys[selected], "ctx", split_axis=0, concat_axis=2, tiled=True),
        lax.all_to_all(held_values[selected], "ctx", split_axis=0, concat_axis=2, tiled=True),
    )
    fine_keys = got_keys.reshape(tiles_here, SEL * TILE, columns)
    fine_values = got_values.reshape(tiles_here, SEL * TILE, columns)
    out_tiles, query_tiles, key_listed, value_listed = ([], [], [], [])
    keys_all = jnp.concatenate([pool_keys, fine_keys[0]], axis=0)
    values_all = jnp.concatenate([pool_values, fine_values[0]], axis=0)
    out_rows, query_grad, key_terms, value_terms = attend(
        query_rows, out_grad, keys_all, values_all
    )
    out_tiles.append(out_rows)
    query_tiles.append(query_grad)
    coarse_keys = key_terms[:comp_count]
    coarse_values = value_terms[:comp_count]
    key_listed.append(key_terms[comp_count:].astype(jnp.bfloat16))
    value_listed.append(value_terms[comp_count:].astype(jnp.bfloat16))
    own_coarse_keys, own_coarse_values = (
        lax.psum_scatter(coarse_keys, "ctx", scatter_dimension=0, tiled=True),
        lax.psum_scatter(coarse_values, "ctx", scatter_dimension=0, tiled=True),
    )
    listed_keys = jnp.stack(key_listed).reshape(tiles_here * SEL, devices, spread, columns)
    listed_values = jnp.stack(value_listed).reshape(tiles_here * SEL, devices, spread, columns)
    back_keys, back_values = (
        lax.all_to_all(listed_keys, "ctx", split_axis=1, concat_axis=0, tiled=True),
        lax.all_to_all(listed_values, "ctx", split_axis=1, concat_axis=0, tiled=True),
    )
    tile_ids = jnp.arange(selected.shape[0], dtype=jnp.int32)[:, None]
    member = (selected.reshape(1, -1) == tile_ids).astype(jnp.bfloat16)
    entries = member.shape[1]
    sum_keys = jnp.dot(
        member, back_keys.reshape(entries, spread * columns), preferred_element_type=jnp.float32
    )
    sum_values = jnp.dot(
        member, back_values.reshape(entries, spread * columns), preferred_element_type=jnp.float32
    )
    held_key_grad = sum_keys.astype(jnp.bfloat16).reshape(devices, tiles_here, spread, columns)
    held_value_grad = sum_values.astype(jnp.bfloat16).reshape(devices, tiles_here, spread, columns)
    owned_keys, owned_values = (
        lax.all_to_all(held_key_grad, "ctx", split_axis=0, concat_axis=2, tiled=True),
        lax.all_to_all(held_value_grad, "ctx", split_axis=0, concat_axis=2, tiled=True),
    )
    grad_key = (
        owned_keys.reshape(height, columns).astype(jnp.float32)
        + jnp.repeat(own_coarse_keys, POOL, axis=0) / POOL
    ).astype(jnp.bfloat16)
    grad_value = (
        owned_values.reshape(height, columns).astype(jnp.float32)
        + jnp.repeat(own_coarse_values, POOL, axis=0) / POOL
    ).astype(jnp.bfloat16)
    attended = out_tiles[0]
    grad_query = query_tiles[0]
    return (attended, grad_query, grad_key, grad_value, own_coarse_keys, own_coarse_values)


SLOTS = 2
CORES_HERE = CORES * PAIR


def remote(src, dst, sent, got, target):
    return pltpu.make_async_remote_copy(
        src_ref=src,
        dst_ref=dst,
        send_sem=sent,
        recv_sem=got,
        device_id={"ctx": target},
        device_id_type=pl.DeviceIdType.MESH,
    )


def wait_for(ref, semaphore):
    pltpu.make_async_copy(ref, ref, semaphore).wait()


def block(index, size):
    return pl.ds(pl.multiple_of(index * size, size), size)


def meet(devices, me):
    barrier = pltpu.get_barrier_semaphore()
    for k in range(1, devices):
        pl.semaphore_signal(
            barrier,
            inc=1,
            device_id={"ctx": lax.rem(me + k, devices)},
            device_id_type=pl.DeviceIdType.MESH,
        )
    pl.semaphore_wait(barrier, devices - 1)


def fused_kernel(devices, chosen_ref, k_ref, v_ref, q_ref, g_ref,
                 ro_ref, rq_ref, rk_ref, rv_ref, rc_ref,
                 keys_in, values_in, queries, grads, out_o, out_q, out_k, out_v, out_c,
                 joined, joined_pool, keys_t, keys_pool, values_t, values_pool, pairs, kept,
                 kept_pool, total, place_ref, spot, chosen_sem,
                 send_in, kv_sem, own_sem, q_sem, g_sem, send_out, back_sem, own_out):
    me = lax.axis_index("ctx")
    levels = devices // CORES_HERE
    per_level = HEADS // levels
    tokens = devices * TILE
    pools = tokens // POOL
    per_tile = TILE // POOL
    listed_rows = SEL * TILE
    level = me // CORES_HERE
    upper = level // 2
    near = (1 - upper) * level + upper * (levels - 1 - level)
    extra_at = CORES * (level % PAIR) + CORES - 1
    two = me % CORES_HERE == extra_at
    apart = me % CORES_HERE - extra_at
    count = 1 + (CORES_HERE * CORES_HERE - apart * apart) // (CORES_HERE * CORES_HERE)
    scaling = HEAD_DIM ** (-0.5)
    rate = scaling * math.log2(math.e)

    def level_at(step):
        turn = step + near * (1 - step // 2) * (1 - 2 * step)
        return (1 - upper) * turn + upper * (levels - 1 - turn)

    meet(devices, me)

    my_rows = block(me, TILE)

    def send_pair(index):
        def step(i, carry):
            goal = level_at(i // per_level)
            j = lax.rem(i + me, per_level)
            spare = j // CORES_HERE
            owner = (
                goal * CORES_HERE
                + (1 - spare) * j
                + spare * (CORES * (goal % PAIR) + CORES - 1)
            )
            columns = block(goal * per_level + j, HEAD_DIM)
            if index == 0:
                moves = [
                    (k_ref, keys_in.at[spare, my_rows, :], kv_sem.at[0, spare]),
                    (v_ref, values_in.at[spare, my_rows, :], kv_sem.at[1, spare]),
                ]
            else:
                moves = [
                    (q_ref, queries.at[spare, my_rows, :], q_sem.at[spare, me]),
                    (g_ref, grads.at[spare, my_rows, :], g_sem.at[spare, me]),
                ]

            @pl.when(owner != me)
            def _():
                for n, (src, dst, got) in enumerate(moves):
                    remote(src.at[:, columns], dst, send_in.at[2 * index + n], got, owner).start()

            @pl.when(owner == me)
            def _():
                for n, (src, dst, got) in enumerate(moves):
                    arrived = own_sem.at[n, spare] if index == 0 else got
                    pltpu.make_async_copy(src.at[:, columns], dst, arrived).start()

            return carry

        lax.fori_loop(0, HEADS, step, 0)

    chosen = pltpu.make_async_copy(chosen_ref, place_ref, chosen_sem)
    chosen.start()
    send_pair(0)
    send_pair(1)
    chosen.wait()

    def find(t, carry):
        for u in range(devices):
            at = SEL
            for j in range(SEL):
                at = jnp.where(place_ref[j, t] == u, j, at)
            spot[t, u] = at
        return carry

    lax.fori_loop(0, devices, find, 0)

    for i in range(CORES_HERE):
        kept[i, SEL] = jnp.zeros((TILE, 2 * HEAD_DIM), jnp.bfloat16)

    def send_back(slot, tile, moves):
        @pl.when(tile != me)
        def _():
            for a, src, dst in moves:
                remote(src, dst, send_out.at[a, slot], back_sem.at[a], tile).start()

        @pl.when(tile == me)
        def _():
            for a, src, dst in moves:
                pltpu.make_async_copy(src, dst, own_out.at[a, slot]).start()

    def run_head(slot, carry):
        head = level * per_level + (1 - slot) * (me % CORES_HERE) + slot * CORES_HERE
        columns = block(head, HEAD_DIM)

        def send_rows(tile):
            rows = block(tile, TILE)
            send_back(
                slot,
                tile,
                [
                    (0, out_o.at[slot, rows, :], ro_ref.at[:, columns]),
                    (1, out_q.at[slot, rows, :], rq_ref.at[:, columns]),
                ],
            )

        for n, (source, turned, turned_pool) in enumerate(
            ((keys_in, keys_t, keys_pool), (values_in, values_t, values_pool))
        ):
            wait_for(source.at[slot, pl.ds(0, tokens - TILE), :], kv_sem.at[n, slot])
            wait_for(source.at[slot, my_rows, :], own_sem.at[n, slot])
            part = slice(n * HEAD_DIM, (n + 1) * HEAD_DIM)
            rows = source[slot]
            means = jnp.sum(rows.astype(jnp.float32).reshape(pools, POOL, HEAD_DIM), axis=1)
            means = (means * (1.0 / POOL)).astype(jnp.bfloat16)
            joined_pool[:, part] = means
            turned_pool[...] = means.T
            for tile in range(devices):
                one = rows[tile * TILE : (tile + 1) * TILE]
                joined[tile, :, part] = one
                turned[tile] = one.T
        total[...] = jnp.zeros_like(total)

        def tile_step(n, carry):
            i = lax.rem(n, CORES_HERE)
            t = level_at(n // CORES_HERE) * CORES_HERE + i
            rows = block(t, TILE)

            @pl.when(n > 0)
            def _():
                before = n - 1
                send_rows(
                    level_at(before // CORES_HERE) * CORES_HERE + lax.rem(before, CORES_HERE)
                )

            wait_for(queries.at[slot, rows, :], q_sem.at[slot, t])
            wait_for(grads.at[slot, rows, :], g_sem.at[slot, t])
            query = queries[slot, rows, :]
            grad = grads[slot, rows, :]
            blank = jnp.zeros_like(query)
            paired = jnp.concatenate(
                [
                    jnp.concatenate([query, blank], axis=1),
                    jnp.concatenate([blank, grad], axis=1),
                ],
                axis=0,
            )
            pairs[i] = paired
            places = [place_ref[j, t] for j in range(SEL)]
            listed = jnp.concatenate(
                [joined[place] for place in places] + [joined_pool[...]], axis=0
            )
            both = contract(listed, paired, 1, 1)
            scores = both[:, :TILE]
            prob_grad = both[:, TILE:]
            summit = jnp.max(scores, axis=0, keepdims=True)
            raised = jnp.exp2((scores - summit) * rate)
            scale = 1.0 / jnp.sum(raised, axis=0, keepdims=True)
            dots = jnp.sum(raised * prob_grad, axis=0, keepdims=True) * scale
            weights = raised * scale
            score_grad = (weights * (prob_grad - dots)).astype(jnp.bfloat16)
            rounded = weights.astype(jnp.bfloat16)
            for part, values in ((0, score_grad), (HEAD_DIM, rounded)):
                for j in range(SEL):
                    kept[i, j, :, part : part + HEAD_DIM] = values[j * TILE : (j + 1) * TILE]
                kept_pool[i, :, part : part + HEAD_DIM] = values[listed_rows:]
            listed_kt = jnp.concatenate(
                [keys_t[place] for place in places] + [keys_pool[...]], axis=1
            )
            listed_vt = jnp.concatenate(
                [values_t[place] for place in places] + [values_pool[...]], axis=1
            )
            out_t = jnp.dot(listed_vt, rounded, preferred_element_type=jnp.float32)
            dq_t = jnp.dot(listed_kt, score_grad, preferred_element_type=jnp.float32) * scaling
            out_o[slot, rows, :] = out_t.T.astype(jnp.bfloat16)
            out_q[slot, rows, :] = dq_t.T.astype(jnp.bfloat16)
            return carry

        def add_terms(g, carry):
            first = level_at(g) * CORES_HERE
            facing = pairs[...].reshape(CORES_HERE * 2 * TILE, 2 * HEAD_DIM)
            for u in range(devices):
                found = jnp.concatenate(
                    [kept[i, spot[first + i, u]] for i in range(CORES_HERE)],
                    axis=1,
                )
                total[u * TILE : (u + 1) * TILE, :] += jnp.dot(
                    found, facing, preferred_element_type=jnp.float32
                )
            found = jnp.concatenate([kept_pool[i] for i in range(CORES_HERE)], axis=1)
            total[tokens:, :] += jnp.dot(found, facing, preferred_element_type=jnp.float32)
            return carry

        def group_step(g, carry):
            lax.fori_loop(g * CORES_HERE, (g + 1) * CORES_HERE, tile_step, 0)
            return add_terms(g, carry)

        lax.fori_loop(0, levels, group_step, 0)
        send_rows(level_at(levels - 1) * CORES_HERE + CORES_HERE - 1)
        for ref, at, factor in ((out_k, 0, scaling), (out_v, HEAD_DIM, 1.0)):
            coarse = total[tokens:, at : at + HEAD_DIM] * factor
            fine = total[:tokens, at : at + HEAD_DIM] * factor
            fine = fine.reshape(pools, POOL, HEAD_DIM) + (coarse * (1.0 / POOL))[:, None, :]
            ref[slot] = fine.reshape(tokens, HEAD_DIM).astype(jnp.bfloat16)
            start = 0 if at == 0 else per_tile
            for tile in range(devices):
                out_c[slot, tile, start : start + per_tile, :] = coarse[
                    tile * per_tile : (tile + 1) * per_tile
                ]

        def send_sums(n, carry):
            tile = level_at(n // CORES_HERE) * CORES_HERE + lax.rem(n, CORES_HERE)
            rows = block(tile, TILE)
            send_back(
                slot,
                tile,
                [
                    (2, out_k.at[slot, rows, :], rk_ref.at[:, columns]),
                    (3, out_v.at[slot, rows, :], rv_ref.at[:, columns]),
                    (4, out_c.at[slot, tile], rc_ref.at[head]),
                ],
            )
            return carry

        lax.fori_loop(0, devices, send_sums, 0)
        return carry

    lax.fori_loop(0, count, run_head, 0)

    stores = (out_o, out_q, out_k, out_v)
    landed = (ro_ref, rq_ref, rk_ref, rv_ref)

    def sent(slot):
        for a, ref in enumerate(stores):
            wait_for(ref.at[slot, pl.ds(0, tokens - TILE), :], send_out.at[a, slot])
            wait_for(ref.at[slot, my_rows, :], own_out.at[a, slot])
        wait_for(out_c.at[slot, pl.ds(0, devices - 1)], send_out.at[4, slot])
        wait_for(out_c.at[slot, me], own_out.at[4, slot])

    def finish(own):
        for n, ref in enumerate((k_ref, v_ref, q_ref, g_ref)):
            wait_for(ref.at[:, pl.ds(0, (HEADS - own) * HEAD_DIM)], send_in.at[n])
        for a, ref in enumerate(landed):
            wait_for(ref.at[:, pl.ds(0, (HEADS - own) * HEAD_DIM)], back_sem.at[a])
        wait_for(rc_ref.at[pl.ds(0, HEADS - own)], back_sem.at[4])

    sent(0)

    @pl.when(two)
    def _():
        sent(1)
        finish(2)

    @pl.when(jnp.logical_not(two))
    def _():
        finish(1)


def fused(selected, arrays, devices):
    turned_list = selected.T
    tokens = devices * TILE
    pools = tokens // POOL
    flat = jax.ShapeDtypeStruct((TILE, HEADS * HEAD_DIM), jnp.bfloat16)
    coarse = jax.ShapeDtypeStruct((HEADS, 2 * TILE // POOL, HEAD_DIM), jnp.float32)
    slabs = pltpu.VMEM((SLOTS, tokens, HEAD_DIM), jnp.bfloat16)
    turned = pltpu.VMEM((devices, HEAD_DIM, TILE), jnp.bfloat16)
    turned_pool = pltpu.VMEM((HEAD_DIM, pools), jnp.bfloat16)
    return pl.pallas_call(
        functools.partial(fused_kernel, devices),
        out_shape=[flat] * 4 + [coarse],
        in_specs=[pl.BlockSpec(memory_space=pl.ANY)] * 5,
        out_specs=[pl.BlockSpec(memory_space=pl.ANY)] * 5,
        scratch_shapes=[
            slabs,
            slabs,
            slabs,
            slabs,
            slabs,
            slabs,
            slabs,
            slabs,
            pltpu.VMEM((SLOTS, devices, 2 * TILE // POOL, HEAD_DIM), jnp.float32),
            pltpu.VMEM((devices, TILE, 2 * HEAD_DIM), jnp.bfloat16),
            pltpu.VMEM((pools, 2 * HEAD_DIM), jnp.bfloat16),
            turned,
            turned_pool,
            turned,
            turned_pool,
            pltpu.VMEM((CORES_HERE, 2 * TILE, 2 * HEAD_DIM), jnp.bfloat16),
            pltpu.VMEM((CORES_HERE, SEL + 1, TILE, 2 * HEAD_DIM), jnp.bfloat16),
            pltpu.VMEM((CORES_HERE, pools, 2 * HEAD_DIM), jnp.bfloat16),
            pltpu.VMEM((tokens + pools, 2 * HEAD_DIM), jnp.float32),
            pltpu.SMEM(turned_list.shape, jnp.int32),
            pltpu.SMEM((devices, devices), jnp.int32),
            pltpu.SemaphoreType.DMA,
            pltpu.SemaphoreType.DMA((4,)),
            pltpu.SemaphoreType.DMA((2, SLOTS)),
            pltpu.SemaphoreType.DMA((2, SLOTS)),
            pltpu.SemaphoreType.DMA((SLOTS, devices)),
            pltpu.SemaphoreType.DMA((SLOTS, devices)),
            pltpu.SemaphoreType.DMA((5, SLOTS)),
            pltpu.SemaphoreType.DMA((5,)),
            pltpu.SemaphoreType.DMA((5, SLOTS)),
        ],
        compiler_params=pltpu.CompilerParams(collective_id=0, has_side_effects=True),
        name="exchange_heads",
    )(turned_list, *arrays)


def place_kernel(pieces, a_ref, b_ref, c_ref, d_ref, coarse_ref,
                 oa_ref, ob_ref, oc_ref, od_ref, keys_ref, values_ref, held, in_sem, out_sem):
    sources = (a_ref, b_ref, c_ref, d_ref)
    targets = (oa_ref, ob_ref, oc_ref, od_ref)
    height = a_ref.shape[0] // pieces
    steps = [(n, p) for p in range(pieces) for n in range(4)]

    def move(n, p, out):
        rows = pl.ds(p * height, height)
        here = held.at[n, rows, :]
        if out:
            return pltpu.make_async_copy(here, targets[n].at[rows, :], out_sem.at[n, p])
        return pltpu.make_async_copy(sources[n].at[rows, :], here, in_sem.at[n, p])

    for n, p in steps:
        move(n, p, False).start()
    per_tile = TILE // POOL
    for head in range(HEADS):
        columns = slice(head * HEAD_DIM, (head + 1) * HEAD_DIM)
        keys_ref[:, columns] = coarse_ref[head, :per_tile]
        values_ref[:, columns] = coarse_ref[head, per_tile:]
    for n, p in steps:
        move(n, p, False).wait()
        move(n, p, True).start()
    for n, p in steps:
        move(n, p, True).wait()


def place(parts, coarse):
    pieces = 2
    shape = jax.ShapeDtypeStruct(parts[0].shape, jnp.bfloat16)
    sums = jax.ShapeDtypeStruct((TILE // POOL, HEADS * HEAD_DIM), jnp.float32)
    anywhere = [pl.BlockSpec(memory_space=pl.ANY)] * 4
    whole = pl.BlockSpec(memory_space=pltpu.VMEM)
    return pl.pallas_call(
        functools.partial(place_kernel, pieces),
        out_shape=[shape] * 4 + [sums] * 2,
        in_specs=anywhere + [whole],
        out_specs=anywhere + [whole] * 2,
        scratch_shapes=[
            pltpu.VMEM((4, *shape.shape), jnp.bfloat16),
            pltpu.SemaphoreType.DMA((4, pieces)),
            pltpu.SemaphoreType.DMA((4, pieces)),
        ],
        name="place",
    )(*parts, coarse)


def exchange_shards(query_rows, key_rows, value_rows, out_grad, selected):
    devices = lax.axis_size("ctx")
    *parts, coarse = fused(selected, (key_rows, value_rows, query_rows, out_grad), devices)
    return tuple(place(parts, coarse))


def shards(query_rows, key_rows, value_rows, out_grad, selected):
    devices = lax.axis_size("ctx")
    fits = devices == 4 * CORES * PAIR and query_rows.shape[0] == TILE
    chosen = exchange_shards if fits else listed_shards
    return chosen(query_rows, key_rows, value_rows, out_grad, selected)


def solution(mesh):
    in_specs = (
        P(("groups", "ctx"), None),
        P(("groups", "ctx"), None),
        P(("groups", "ctx"), None),
        P(("groups", "ctx"), None),
        P("groups", None),
    )
    out_specs = (
        P(("groups", "ctx"), None),
        P(("groups", "ctx"), None),
        P(("groups", "ctx"), None),
        P(("groups", "ctx"), None),
        P(("groups", "ctx"), None),
        P(("groups", "ctx"), None),
    )
    return jax.shard_map(shards, mesh=mesh, in_specs=in_specs, out_specs=out_specs, check_vma=False)
```

```python
import functools
import math

import jax
import jax.numpy as jnp
from jax import lax
from jax.experimental import pallas as pl
from jax.experimental.pallas import tpu as pltpu
from jax.sharding import PartitionSpec as P

HEADS = 20
HEAD_DIM = 128
TILE = 128
POOL = 64
SEL = 8
CORES = 2
PAIR = 2


def pooled(rows):
    return jnp.mean(rows.astype(jnp.float32).reshape(-1, POOL, rows.shape[1]), axis=1).astype(
        jnp.bfloat16
    )


def contract(left, right, left_dim, right_dim):
    return lax.dot_general(
        left, right, (((left_dim,), (right_dim,)), ((), ())), preferred_element_type=jnp.float32
    )


def attend(queries, grads_out, keys_all, values_all):
    scaling = HEAD_DIM ** (-0.5)
    out_parts, query_parts, key_parts, value_parts = ([], [], [], [])
    for head in range(HEADS):
        lower = head * HEAD_DIM
        upper = lower + HEAD_DIM
        head_query = queries[:, lower:upper]
        head_grad = grads_out[:, lower:upper]
        head_key = keys_all[:, lower:upper]
        head_value = values_all[:, lower:upper]
        scores = contract(head_query, head_key, 1, 1) * scaling
        summit = jnp.max(scores, axis=-1, keepdims=True)
        raised = jnp.exp(scores - summit)
        weights = raised / jnp.sum(raised, axis=-1, keepdims=True)
        rounded = weights.astype(jnp.bfloat16)
        out_rows = jnp.dot(rounded, head_value, preferred_element_type=jnp.float32).astype(
            jnp.bfloat16
        )
        row_dots = jnp.sum(
            head_grad.astype(jnp.float32) * out_rows.astype(jnp.float32), axis=-1, keepdims=True
        )
        prob_grad = contract(head_grad, head_value, 1, 1)
        score_grad = (weights * (prob_grad - row_dots)).astype(jnp.bfloat16)
        query_grad = jnp.dot(score_grad, head_key, preferred_element_type=jnp.float32) * scaling
        key_terms = contract(score_grad, head_query, 0, 0) * scaling
        value_terms = contract(rounded, head_grad, 0, 0)
        out_parts.append(out_rows)
        query_parts.append(query_grad.astype(jnp.bfloat16))
        key_parts.append(key_terms)
        value_parts.append(value_terms)
    return (
        jnp.concatenate(out_parts, axis=1),
        jnp.concatenate(query_parts, axis=1),
        jnp.concatenate(key_parts, axis=1),
        jnp.concatenate(value_parts, axis=1),
    )


def package(tiles_in, pooled_in, devices, spread):
    tiles_here, tile_len, columns = tiles_in.shape
    per_tile = tile_len // POOL
    split_rows = tiles_in.reshape(tiles_here, devices, spread, columns)
    copies = jnp.broadcast_to(
        pooled_in.reshape(tiles_here, 1, per_tile, columns),
        (tiles_here, devices, per_tile, columns),
    )
    return jnp.concatenate([split_rows, copies], axis=2).reshape(
        tiles_here, devices * (spread + per_tile), columns
    )


def listed_shards(query_rows, key_rows, value_rows, out_grad, selected):
    height, columns = query_rows.shape
    devices = lax.axis_size("ctx")
    tiles_here = height // TILE
    spread = TILE // devices
    own_keys = pooled(key_rows)
    own_values = pooled(value_rows)
    key_tiles = key_rows.reshape(tiles_here, TILE, columns)
    value_tiles = value_rows.reshape(tiles_here, TILE, columns)
    joined_keys, joined_values = (
        lax.all_to_all(
            package(key_tiles, own_keys, devices, spread),
            "ctx",
            split_axis=1,
            concat_axis=0,
            tiled=True,
        ),
        lax.all_to_all(
            package(value_tiles, own_values, devices, spread),
            "ctx",
            split_axis=1,
            concat_axis=0,
            tiled=True,
        ),
    )
    held_keys = joined_keys[:, :spread]
    held_values = joined_values[:, :spread]
    pool_keys = joined_keys[:, spread:].reshape(-1, columns)
    pool_values = joined_values[:, spread:].reshape(-1, columns)
    comp_count = pool_keys.shape[0]
    got_keys, got_values = (
        lax.all_to_all(held_keys[selected], "ctx", split_axis=0, concat_axis=2, tiled=True),
        lax.all_to_all(held_values[selected], "ctx", split_axis=0, concat_axis=2, tiled=True),
    )
    fine_keys = got_keys.reshape(tiles_here, SEL * TILE, columns)
    fine_values = got_values.reshape(tiles_here, SEL * TILE, columns)
    out_tiles, query_tiles, key_listed, value_listed = ([], [], [], [])
    keys_all = jnp.concatenate([pool_keys, fine_keys[0]], axis=0)
    values_all = jnp.concatenate([pool_values, fine_values[0]], axis=0)
    out_rows, query_grad, key_terms, value_terms = attend(
        query_rows, out_grad, keys_all, values_all
    )
    out_tiles.append(out_rows)
    query_tiles.append(query_grad)
    coarse_keys = key_terms[:comp_count]
    coarse_values = value_terms[:comp_count]
    key_listed.append(key_terms[comp_count:].astype(jnp.bfloat16))
    value_listed.append(value_terms[comp_count:].astype(jnp.bfloat16))
    own_coarse_keys, own_coarse_values = (
        lax.psum_scatter(coarse_keys, "ctx", scatter_dimension=0, tiled=True),
        lax.psum_scatter(coarse_values, "ctx", scatter_dimension=0, tiled=True),
    )
    listed_keys = jnp.stack(key_listed).reshape(tiles_here * SEL, devices, spread, columns)
    listed_values = jnp.stack(value_listed).reshape(tiles_here * SEL, devices, spread, columns)
    back_keys, back_values = (
        lax.all_to_all(listed_keys, "ctx", split_axis=1, concat_axis=0, tiled=True),
        lax.all_to_all(listed_values, "ctx", split_axis=1, concat_axis=0, tiled=True),
    )
    tile_ids = jnp.arange(selected.shape[0], dtype=jnp.int32)[:, None]
    member = (selected.reshape(1, -1) == tile_ids).astype(jnp.bfloat16)
    entries = member.shape[1]
    sum_keys = jnp.dot(
        member, back_keys.reshape(entries, spread * columns), preferred_element_type=jnp.float32
    )
    sum_values = jnp.dot(
        member, back_values.reshape(entries, spread * columns), preferred_element_type=jnp.float32
    )
    held_key_grad = sum_keys.astype(jnp.bfloat16).reshape(devices, tiles_here, spread, columns)
    held_value_grad = sum_values.astype(jnp.bfloat16).reshape(devices, tiles_here, spread, columns)
    owned_keys, owned_values = (
        lax.all_to_all(held_key_grad, "ctx", split_axis=0, concat_axis=2, tiled=True),
        lax.all_to_all(held_value_grad, "ctx", split_axis=0, concat_axis=2, tiled=True),
    )
    grad_key = (
        owned_keys.reshape(height, columns).astype(jnp.float32)
        + jnp.repeat(own_coarse_keys, POOL, axis=0) / POOL
    ).astype(jnp.bfloat16)
    grad_value = (
        owned_values.reshape(height, columns).astype(jnp.float32)
        + jnp.repeat(own_coarse_values, POOL, axis=0) / POOL
    ).astype(jnp.bfloat16)
    attended = out_tiles[0]
    grad_query = query_tiles[0]
    return (attended, grad_query, grad_key, grad_value, own_coarse_keys, own_coarse_values)


SLOTS = 2
CORES_HERE = CORES * PAIR


def remote(src, dst, sent, got, target):
    return pltpu.make_async_remote_copy(
        src_ref=src,
        dst_ref=dst,
        send_sem=sent,
        recv_sem=got,
        device_id={"ctx": target},
        device_id_type=pl.DeviceIdType.MESH,
    )


def wait_for(ref, semaphore):
    pltpu.make_async_copy(ref, ref, semaphore).wait()


def block(index, size):
    return pl.ds(pl.multiple_of(index * size, size), size)


def meet(devices, me):
    barrier = pltpu.get_barrier_semaphore()
    for k in range(1, devices):
        pl.semaphore_signal(
            barrier,
            inc=1,
            device_id={"ctx": lax.rem(me + k, devices)},
            device_id_type=pl.DeviceIdType.MESH,
        )
    pl.semaphore_wait(barrier, devices - 1)


def fused_kernel(devices, chosen_ref, k_ref, v_ref, q_ref, g_ref,
                 ro_ref, rq_ref, rk_ref, rv_ref, rc_ref,
                 keys_in, values_in, queries, grads, out_o, out_q, out_k, out_v, out_c,
                 joined, joined_pool, keys_t, keys_pool, values_t, values_pool, pairs, kept,
                 kept_pool, total, place_ref, spot, chosen_sem,
                 send_in, kv_sem, own_sem, q_sem, g_sem, send_out, back_sem, own_out):
    me = lax.axis_index("ctx")
    levels = devices // CORES_HERE
    per_level = HEADS // levels
    tokens = devices * TILE
    pools = tokens // POOL
    per_tile = TILE // POOL
    listed_rows = SEL * TILE
    level = me // CORES_HERE
    upper = level // 2
    near = (1 - upper) * level + upper * (levels - 1 - level)
    extra_at = CORES * (level % PAIR) + CORES - 1
    two = me % CORES_HERE == extra_at
    apart = me % CORES_HERE - extra_at
    count = 1 + (CORES_HERE * CORES_HERE - apart * apart) // (CORES_HERE * CORES_HERE)
    scaling = HEAD_DIM ** (-0.5)
    rate = scaling * math.log2(math.e)

    def level_at(step):
        turn = step + near * (1 - step // 2) * (1 - 2 * step)
        return (1 - upper) * turn + upper * (levels - 1 - turn)

    meet(devices, me)

    my_rows = block(me, TILE)

    def send_pair(index):
        def step(i, carry):
            goal = level_at(i // per_level)
            j = lax.rem(i + me, per_level)
            spare = j // CORES_HERE
            owner = (
                goal * CORES_HERE
                + (1 - spare) * j
                + spare * (CORES * (goal % PAIR) + CORES - 1)
            )
            columns = block(goal * per_level + j, HEAD_DIM)
            if index == 0:
                moves = [
                    (k_ref, keys_in.at[spare, my_rows, :], kv_sem.at[0, spare]),
                    (v_ref, values_in.at[spare, my_rows, :], kv_sem.at[1, spare]),
                ]
            else:
                moves = [
                    (q_ref, queries.at[spare, my_rows, :], q_sem.at[spare, me]),
                    (g_ref, grads.at[spare, my_rows, :], g_sem.at[spare, me]),
                ]

            @pl.when(owner != me)
            def _():
                for n, (src, dst, got) in enumerate(moves):
                    remote(src.at[:, columns], dst, send_in.at[2 * index + n], got, owner).start()

            @pl.when(owner == me)
            def _():
                for n, (src, dst, got) in enumerate(moves):
                    arrived = own_sem.at[n, spare] if index == 0 else got
                    pltpu.make_async_copy(src.at[:, columns], dst, arrived).start()

            return carry

        lax.fori_loop(0, HEADS, step, 0)

    chosen = pltpu.make_async_copy(chosen_ref, place_ref, chosen_sem)
    chosen.start()
    send_pair(0)
    send_pair(1)
    chosen.wait()

    def find(t, carry):
        for u in range(devices):
            at = SEL
            for j in range(SEL):
                at = jnp.where(place_ref[j, t] == u, j, at)
            spot[t, u] = at
        return carry

    lax.fori_loop(0, devices, find, 0)

    for i in range(CORES_HERE):
        kept[i, SEL] = jnp.zeros((TILE, 2 * HEAD_DIM), jnp.bfloat16)

    def send_back(slot, tile, moves):
        @pl.when(tile != me)
        def _():
            for a, src, dst in moves:
                remote(src, dst, send_out.at[a, slot], back_sem.at[a], tile).start()

        @pl.when(tile == me)
        def _():
            for a, src, dst in moves:
                pltpu.make_async_copy(src, dst, own_out.at[a, slot]).start()

    def run_head(slot, carry):
        head = level * per_level + (1 - slot) * (me % CORES_HERE) + slot * CORES_HERE
        columns = block(head, HEAD_DIM)

        def send_rows(tile):
            rows = block(tile, TILE)
            send_back(
                slot,
                tile,
                [
                    (0, out_o.at[slot, rows, :], ro_ref.at[:, columns]),
                    (1, out_q.at[slot, rows, :], rq_ref.at[:, columns]),
                ],
            )

        for n, (source, turned, turned_pool) in enumerate(
            ((keys_in, keys_t, keys_pool), (values_in, values_t, values_pool))
        ):
            wait_for(source.at[slot, pl.ds(0, tokens - TILE), :], kv_sem.at[n, slot])
            wait_for(source.at[slot, my_rows, :], own_sem.at[n, slot])
            part = slice(n * HEAD_DIM, (n + 1) * HEAD_DIM)
            rows = source[slot]
            means = jnp.sum(rows.astype(jnp.float32).reshape(pools, POOL, HEAD_DIM), axis=1)
            means = (means * (1.0 / POOL)).astype(jnp.bfloat16)
            joined_pool[:, part] = means
            turned_pool[...] = means.T
            for tile in range(devices):
                one = rows[tile * TILE : (tile + 1) * TILE]
                joined[tile, :, part] = one
                turned[tile] = one.T
        total[...] = jnp.zeros_like(total)

        def tile_step(n, carry):
            i = lax.rem(n, CORES_HERE)
            t = level_at(n // CORES_HERE) * CORES_HERE + i
            rows = block(t, TILE)

            @pl.when(n > 0)
            def _():
                before = n - 1
                send_rows(
                    level_at(before // CORES_HERE) * CORES_HERE + lax.rem(before, CORES_HERE)
                )

            wait_for(queries.at[slot, rows, :], q_sem.at[slot, t])
            wait_for(grads.at[slot, rows, :], g_sem.at[slot, t])
            query = queries[slot, rows, :]
            grad = grads[slot, rows, :]
            blank = jnp.zeros_like(query)
            paired = jnp.concatenate(
                [
                    jnp.concatenate([query, blank], axis=1),
                    jnp.concatenate([blank, grad], axis=1),
                ],
                axis=0,
            )
            pairs[i] = paired
            places = [place_ref[j, t] for j in range(SEL)]
            listed = jnp.concatenate(
                [joined[place] for place in places] + [joined_pool[...]], axis=0
            )
            both = contract(listed, paired, 1, 1)
            scores = both[:, :TILE]
            prob_grad = both[:, TILE:]
            summit = jnp.max(scores, axis=0, keepdims=True)
            raised = jnp.exp2((scores - summit) * rate)
            scale = 1.0 / jnp.sum(raised, axis=0, keepdims=True)
            dots = jnp.sum(raised * prob_grad, axis=0, keepdims=True) * scale
            weights = raised * scale
            score_grad = (weights * (prob_grad - dots)).astype(jnp.bfloat16)
            rounded = weights.astype(jnp.bfloat16)
            for part, values in ((0, score_grad), (HEAD_DIM, rounded)):
                for j in range(SEL):
                    kept[i, j, :, part : part + HEAD_DIM] = values[j * TILE : (j + 1) * TILE]
                kept_pool[i, :, part : part + HEAD_DIM] = values[listed_rows:]
            listed_kt = jnp.concatenate(
                [keys_t[place] for place in places] + [keys_pool[...]], axis=1
            )
            listed_vt = jnp.concatenate(
                [values_t[place] for place in places] + [values_pool[...]], axis=1
            )
            out_t = jnp.dot(listed_vt, rounded, preferred_element_type=jnp.float32)
            dq_t = jnp.dot(listed_kt, score_grad, preferred_element_type=jnp.float32) * scaling
            out_o[slot, rows, :] = out_t.T.astype(jnp.bfloat16)
            out_q[slot, rows, :] = dq_t.T.astype(jnp.bfloat16)
            return carry

        def add_terms(g, carry):
            first = level_at(g) * CORES_HERE
            facing = pairs[...].reshape(CORES_HERE * 2 * TILE, 2 * HEAD_DIM)
            for u in range(devices):
                found = jnp.concatenate(
                    [kept[i, spot[first + i, u]] for i in range(CORES_HERE)],
                    axis=1,
                )
                total[u * TILE : (u + 1) * TILE, :] += jnp.dot(
                    found, facing, preferred_element_type=jnp.float32
                )
            found = jnp.concatenate([kept_pool[i] for i in range(CORES_HERE)], axis=1)
            total[tokens:, :] += jnp.dot(found, facing, preferred_element_type=jnp.float32)
            return carry

        def group_step(g, carry):
            lax.fori_loop(g * CORES_HERE, (g + 1) * CORES_HERE, tile_step, 0)
            return add_terms(g, carry)

        lax.fori_loop(0, levels, group_step, 0)
        send_rows(level_at(levels - 1) * CORES_HERE + CORES_HERE - 1)
        for ref, at, factor in ((out_k, 0, scaling), (out_v, HEAD_DIM, 1.0)):
            coarse = total[tokens:, at : at + HEAD_DIM] * factor
            fine = total[:tokens, at : at + HEAD_DIM] * factor
            fine = fine.reshape(pools, POOL, HEAD_DIM) + (coarse * (1.0 / POOL))[:, None, :]
            ref[slot] = fine.reshape(tokens, HEAD_DIM).astype(jnp.bfloat16)
            start = 0 if at == 0 else per_tile
            for tile in range(devices):
                out_c[slot, tile, start : start + per_tile, :] = coarse[
                    tile * per_tile : (tile + 1) * per_tile
                ]

        def send_sums(n, carry):
            tile = level_at(n // CORES_HERE) * CORES_HERE + lax.rem(n, CORES_HERE)
            rows = block(tile, TILE)
            send_back(
                slot,
                tile,
                [
                    (2, out_k.at[slot, rows, :], rk_ref.at[:, columns]),
                    (3, out_v.at[slot, rows, :], rv_ref.at[:, columns]),
                    (4, out_c.at[slot, tile], rc_ref.at[head]),
                ],
            )
            return carry

        lax.fori_loop(0, devices, send_sums, 0)
        return carry

    lax.fori_loop(0, count, run_head, 0)

    stores = (out_o, out_q, out_k, out_v)
    landed = (ro_ref, rq_ref, rk_ref, rv_ref)

    def sent(slot):
        for a, ref in enumerate(stores):
            wait_for(ref.at[slot, pl.ds(0, tokens - TILE), :], send_out.at[a, slot])
            wait_for(ref.at[slot, my_rows, :], own_out.at[a, slot])
        wait_for(out_c.at[slot, pl.ds(0, devices - 1)], send_out.at[4, slot])
        wait_for(out_c.at[slot, me], own_out.at[4, slot])

    def finish(own):
        for n, ref in enumerate((k_ref, v_ref, q_ref, g_ref)):
            wait_for(ref.at[:, pl.ds(0, (HEADS - own) * HEAD_DIM)], send_in.at[n])
        for a, ref in enumerate(landed):
            wait_for(ref.at[:, pl.ds(0, (HEADS - own) * HEAD_DIM)], back_sem.at[a])
        wait_for(rc_ref.at[pl.ds(0, HEADS - own)], back_sem.at[4])

    sent(0)

    @pl.when(two)
    def _():
        sent(1)
        finish(2)

    @pl.when(jnp.logical_not(two))
    def _():
        finish(1)


def fused(selected, arrays, devices):
    turned_list, *arrays = (
        pltpu.with_memory_space_constraint(part, pltpu.HBM) for part in (selected.T, *arrays)
    )
    tokens = devices * TILE
    pools = tokens // POOL
    flat = pltpu.VMEM((TILE, HEADS * HEAD_DIM), jnp.bfloat16)
    coarse = jax.ShapeDtypeStruct((HEADS, 2 * TILE // POOL, HEAD_DIM), jnp.float32)
    slabs = pltpu.VMEM((SLOTS, tokens, HEAD_DIM), jnp.bfloat16)
    turned = pltpu.VMEM((devices, HEAD_DIM, TILE), jnp.bfloat16)
    turned_pool = pltpu.VMEM((HEAD_DIM, pools), jnp.bfloat16)
    return pl.pallas_call(
        functools.partial(fused_kernel, devices),
        out_shape=[flat] * 4 + [coarse],
        in_specs=[pl.BlockSpec(memory_space=pltpu.HBM)] * 5,
        out_specs=[pl.BlockSpec(memory_space=pltpu.VMEM)] * 4
        + [pl.BlockSpec(memory_space=pl.ANY)],
        scratch_shapes=[
            slabs,
            slabs,
            slabs,
            slabs,
            slabs,
            slabs,
            slabs,
            slabs,
            pltpu.VMEM((SLOTS, devices, 2 * TILE // POOL, HEAD_DIM), jnp.float32),
            pltpu.VMEM((devices, TILE, 2 * HEAD_DIM), jnp.bfloat16),
            pltpu.VMEM((pools, 2 * HEAD_DIM), jnp.bfloat16),
            turned,
            turned_pool,
            turned,
            turned_pool,
            pltpu.VMEM((CORES_HERE, 2 * TILE, 2 * HEAD_DIM), jnp.bfloat16),
            pltpu.VMEM((CORES_HERE, SEL + 1, TILE, 2 * HEAD_DIM), jnp.bfloat16),
            pltpu.VMEM((CORES_HERE, pools, 2 * HEAD_DIM), jnp.bfloat16),
            pltpu.VMEM((tokens + pools, 2 * HEAD_DIM), jnp.float32),
            pltpu.SMEM(turned_list.shape, jnp.int32),
            pltpu.SMEM((devices, devices), jnp.int32),
            pltpu.SemaphoreType.DMA,
            pltpu.SemaphoreType.DMA((4,)),
            pltpu.SemaphoreType.DMA((2, SLOTS)),
            pltpu.SemaphoreType.DMA((2, SLOTS)),
            pltpu.SemaphoreType.DMA((SLOTS, devices)),
            pltpu.SemaphoreType.DMA((SLOTS, devices)),
            pltpu.SemaphoreType.DMA((5, SLOTS)),
            pltpu.SemaphoreType.DMA((5,)),
            pltpu.SemaphoreType.DMA((5, SLOTS)),
        ],
        compiler_params=pltpu.CompilerParams(
            collective_id=0, has_side_effects=True, vmem_limit_bytes=40 * 2**20
        ),
        name="exchange_heads",
    )(turned_list, *arrays)


def place_kernel(a_ref, b_ref, c_ref, d_ref, coarse_ref,
                 oa_ref, ob_ref, oc_ref, od_ref, keys_ref, values_ref, sem):
    moves = [
        pltpu.make_async_copy(source, target, sem.at[n])
        for n, (source, target) in enumerate(
            zip((a_ref, b_ref, c_ref, d_ref), (oa_ref, ob_ref, oc_ref, od_ref))
        )
    ]
    for move in moves:
        move.start()
    per_tile = TILE // POOL
    for head in range(HEADS):
        columns = slice(head * HEAD_DIM, (head + 1) * HEAD_DIM)
        keys_ref[:, columns] = coarse_ref[head, :per_tile]
        values_ref[:, columns] = coarse_ref[head, per_tile:]
    for move in moves:
        move.wait()


def place(parts, coarse):
    shape = jax.ShapeDtypeStruct(parts[0].shape, jnp.bfloat16)
    sums = jax.ShapeDtypeStruct((TILE // POOL, HEADS * HEAD_DIM), jnp.float32)
    whole = pl.BlockSpec(memory_space=pltpu.VMEM)
    parts = [pltpu.with_memory_space_constraint(part, pltpu.VMEM) for part in parts]
    return pl.pallas_call(
        place_kernel,
        out_shape=[shape] * 4 + [sums] * 2,
        in_specs=[whole] * 5,
        out_specs=[pl.BlockSpec(memory_space=pl.ANY)] * 4 + [whole] * 2,
        scratch_shapes=[pltpu.SemaphoreType.DMA((4,))],
        compiler_params=pltpu.CompilerParams(vmem_limit_bytes=2**23),
        name="place",
    )(*parts, coarse)


def exchange_shards(query_rows, key_rows, value_rows, out_grad, selected):
    devices = lax.axis_size("ctx")
    *parts, coarse = fused(selected, (key_rows, value_rows, query_rows, out_grad), devices)
    return tuple(place(parts, coarse))


def shards(query_rows, key_rows, value_rows, out_grad, selected):
    devices = lax.axis_size("ctx")
    fits = devices == 4 * CORES * PAIR and query_rows.shape[0] == TILE
    chosen = exchange_shards if fits else listed_shards
    return chosen(query_rows, key_rows, value_rows, out_grad, selected)


def solution(mesh):
    in_specs = (
        P(("groups", "ctx"), None),
        P(("groups", "ctx"), None),
        P(("groups", "ctx"), None),
        P(("groups", "ctx"), None),
        P("groups", None),
    )
    out_specs = (
        P(("groups", "ctx"), None),
        P(("groups", "ctx"), None),
        P(("groups", "ctx"), None),
        P(("groups", "ctx"), None),
        P(("groups", "ctx"), None),
        P(("groups", "ctx"), None),
    )
    return jax.shard_map(shards, mesh=mesh, in_specs=in_specs, out_specs=out_specs, check_vma=False)
```

```python
import functools
import math

import jax
import jax.numpy as jnp
from jax import lax
from jax.experimental import pallas as pl
from jax.experimental.pallas import tpu as pltpu
from jax.sharding import PartitionSpec as P

HEADS = 20
HEAD_DIM = 128
TILE = 128
POOL = 64
SEL = 8
CORES = 2
PAIR = 2


def pooled(rows):
    return jnp.mean(rows.astype(jnp.float32).reshape(-1, POOL, rows.shape[1]), axis=1).astype(
        jnp.bfloat16
    )


def contract(left, right, left_dim, right_dim):
    return lax.dot_general(
        left, right, (((left_dim,), (right_dim,)), ((), ())), preferred_element_type=jnp.float32
    )


def attend(queries, grads_out, keys_all, values_all):
    scaling = HEAD_DIM ** (-0.5)
    out_parts, query_parts, key_parts, value_parts = ([], [], [], [])
    for head in range(HEADS):
        lower = head * HEAD_DIM
        upper = lower + HEAD_DIM
        head_query = queries[:, lower:upper]
        head_grad = grads_out[:, lower:upper]
        head_key = keys_all[:, lower:upper]
        head_value = values_all[:, lower:upper]
        scores = contract(head_query, head_key, 1, 1) * scaling
        summit = jnp.max(scores, axis=-1, keepdims=True)
        raised = jnp.exp(scores - summit)
        weights = raised / jnp.sum(raised, axis=-1, keepdims=True)
        rounded = weights.astype(jnp.bfloat16)
        out_rows = jnp.dot(rounded, head_value, preferred_element_type=jnp.float32).astype(
            jnp.bfloat16
        )
        row_dots = jnp.sum(
            head_grad.astype(jnp.float32) * out_rows.astype(jnp.float32), axis=-1, keepdims=True
        )
        prob_grad = contract(head_grad, head_value, 1, 1)
        score_grad = (weights * (prob_grad - row_dots)).astype(jnp.bfloat16)
        query_grad = jnp.dot(score_grad, head_key, preferred_element_type=jnp.float32) * scaling
        key_terms = contract(score_grad, head_query, 0, 0) * scaling
        value_terms = contract(rounded, head_grad, 0, 0)
        out_parts.append(out_rows)
        query_parts.append(query_grad.astype(jnp.bfloat16))
        key_parts.append(key_terms)
        value_parts.append(value_terms)
    return (
        jnp.concatenate(out_parts, axis=1),
        jnp.concatenate(query_parts, axis=1),
        jnp.concatenate(key_parts, axis=1),
        jnp.concatenate(value_parts, axis=1),
    )


def package(tiles_in, pooled_in, devices, spread):
    tiles_here, tile_len, columns = tiles_in.shape
    per_tile = tile_len // POOL
    split_rows = tiles_in.reshape(tiles_here, devices, spread, columns)
    copies = jnp.broadcast_to(
        pooled_in.reshape(tiles_here, 1, per_tile, columns),
        (tiles_here, devices, per_tile, columns),
    )
    return jnp.concatenate([split_rows, copies], axis=2).reshape(
        tiles_here, devices * (spread + per_tile), columns
    )


def listed_shards(query_rows, key_rows, value_rows, out_grad, selected):
    height, columns = query_rows.shape
    devices = lax.axis_size("ctx")
    tiles_here = height // TILE
    spread = TILE // devices
    own_keys = pooled(key_rows)
    own_values = pooled(value_rows)
    key_tiles = key_rows.reshape(tiles_here, TILE, columns)
    value_tiles = value_rows.reshape(tiles_here, TILE, columns)
    joined_keys, joined_values = (
        lax.all_to_all(
            package(key_tiles, own_keys, devices, spread),
            "ctx",
            split_axis=1,
            concat_axis=0,
            tiled=True,
        ),
        lax.all_to_all(
            package(value_tiles, own_values, devices, spread),
            "ctx",
            split_axis=1,
            concat_axis=0,
            tiled=True,
        ),
    )
    held_keys = joined_keys[:, :spread]
    held_values = joined_values[:, :spread]
    pool_keys = joined_keys[:, spread:].reshape(-1, columns)
    pool_values = joined_values[:, spread:].reshape(-1, columns)
    comp_count = pool_keys.shape[0]
    got_keys, got_values = (
        lax.all_to_all(held_keys[selected], "ctx", split_axis=0, concat_axis=2, tiled=True),
        lax.all_to_all(held_values[selected], "ctx", split_axis=0, concat_axis=2, tiled=True),
    )
    fine_keys = got_keys.reshape(tiles_here, SEL * TILE, columns)
    fine_values = got_values.reshape(tiles_here, SEL * TILE, columns)
    out_tiles, query_tiles, key_listed, value_listed = ([], [], [], [])
    keys_all = jnp.concatenate([pool_keys, fine_keys[0]], axis=0)
    values_all = jnp.concatenate([pool_values, fine_values[0]], axis=0)
    out_rows, query_grad, key_terms, value_terms = attend(
        query_rows, out_grad, keys_all, values_all
    )
    out_tiles.append(out_rows)
    query_tiles.append(query_grad)
    coarse_keys = key_terms[:comp_count]
    coarse_values = value_terms[:comp_count]
    key_listed.append(key_terms[comp_count:].astype(jnp.bfloat16))
    value_listed.append(value_terms[comp_count:].astype(jnp.bfloat16))
    own_coarse_keys, own_coarse_values = (
        lax.psum_scatter(coarse_keys, "ctx", scatter_dimension=0, tiled=True),
        lax.psum_scatter(coarse_values, "ctx", scatter_dimension=0, tiled=True),
    )
    listed_keys = jnp.stack(key_listed).reshape(tiles_here * SEL, devices, spread, columns)
    listed_values = jnp.stack(value_listed).reshape(tiles_here * SEL, devices, spread, columns)
    back_keys, back_values = (
        lax.all_to_all(listed_keys, "ctx", split_axis=1, concat_axis=0, tiled=True),
        lax.all_to_all(listed_values, "ctx", split_axis=1, concat_axis=0, tiled=True),
    )
    tile_ids = jnp.arange(selected.shape[0], dtype=jnp.int32)[:, None]
    member = (selected.reshape(1, -1) == tile_ids).astype(jnp.bfloat16)
    entries = member.shape[1]
    sum_keys = jnp.dot(
        member, back_keys.reshape(entries, spread * columns), preferred_element_type=jnp.float32
    )
    sum_values = jnp.dot(
        member, back_values.reshape(entries, spread * columns), preferred_element_type=jnp.float32
    )
    held_key_grad = sum_keys.astype(jnp.bfloat16).reshape(devices, tiles_here, spread, columns)
    held_value_grad = sum_values.astype(jnp.bfloat16).reshape(devices, tiles_here, spread, columns)
    owned_keys, owned_values = (
        lax.all_to_all(held_key_grad, "ctx", split_axis=0, concat_axis=2, tiled=True),
        lax.all_to_all(held_value_grad, "ctx", split_axis=0, concat_axis=2, tiled=True),
    )
    grad_key = (
        owned_keys.reshape(height, columns).astype(jnp.float32)
        + jnp.repeat(own_coarse_keys, POOL, axis=0) / POOL
    ).astype(jnp.bfloat16)
    grad_value = (
        owned_values.reshape(height, columns).astype(jnp.float32)
        + jnp.repeat(own_coarse_values, POOL, axis=0) / POOL
    ).astype(jnp.bfloat16)
    attended = out_tiles[0]
    grad_query = query_tiles[0]
    return (attended, grad_query, grad_key, grad_value, own_coarse_keys, own_coarse_values)


SLOTS = 2
CORES_HERE = CORES * PAIR


def remote(src, dst, sent, got, target):
    return pltpu.make_async_remote_copy(
        src_ref=src,
        dst_ref=dst,
        send_sem=sent,
        recv_sem=got,
        device_id={"ctx": target},
        device_id_type=pl.DeviceIdType.MESH,
    )


def wait_for(ref, semaphore):
    pltpu.make_async_copy(ref, ref, semaphore).wait()


def block(index, size):
    return pl.ds(pl.multiple_of(index * size, size), size)


def greet(target):
    pl.semaphore_signal(
        pltpu.get_barrier_semaphore(),
        inc=1,
        device_id={"ctx": target},
        device_id_type=pl.DeviceIdType.MESH,
    )


def fused_kernel(devices, chosen_ref, k_ref, v_ref, q_ref, g_ref,
                 ro_ref, rq_ref, rk_ref, rv_ref, rc_ref,
                 keys_in, values_in, queries, grads, out_o, out_q, out_k, out_v, out_c,
                 joined, joined_pool, keys_t, keys_pool, values_t, values_pool, pairs, kept,
                 kept_pool, total, place_ref, spot, chosen_sem,
                 send_in, kv_sem, own_sem, q_sem, g_sem, send_out, back_sem, own_out):
    me = lax.axis_index("ctx")
    levels = devices // CORES_HERE
    per_level = HEADS // levels
    tokens = devices * TILE
    pools = tokens // POOL
    per_tile = TILE // POOL
    listed_rows = SEL * TILE
    level = me // CORES_HERE
    upper = level // 2
    near = (1 - upper) * level + upper * (levels - 1 - level)
    extra_at = CORES * (level % PAIR) + CORES - 1
    two = me % CORES_HERE == extra_at
    apart = me % CORES_HERE - extra_at
    count = 1 + (CORES_HERE * CORES_HERE - apart * apart) // (CORES_HERE * CORES_HERE)
    scaling = HEAD_DIM ** (-0.5)
    rate = scaling * math.log2(math.e)

    def level_at(step):
        turn = step + near * (1 - 3 * (step // 2) + 2 * (step // 3))
        return (1 - upper) * turn + upper * (levels - 1 - turn)

    barrier = pltpu.get_barrier_semaphore()
    place_here = me % CORES_HERE
    facing_level = levels - 1 - level
    for k in range(CORES_HERE):
        if k:
            greet(level * CORES_HERE + lax.rem(place_here + k, CORES_HERE))
        greet(facing_level * CORES_HERE + k)
    group = 2 * CORES_HERE
    others = [(1 - near) * (1 + up) + near * (levels - 1) * up for up in range(2)]

    @pl.when(near == 1)
    def _():
        pl.semaphore_wait(barrier, group - 1)

    @pl.when(near == 0)
    def _():
        pl.semaphore_wait(barrier, devices - 1)

    for up in range(2):
        for k in range(CORES_HERE):
            greet(others[up] * CORES_HERE + k)

    my_rows = block(me, TILE)

    def send_pair(index, start, end):
        def step(i, carry):
            goal = level_at(i // per_level)
            j = lax.rem(i + me, per_level)
            spare = j // CORES_HERE
            owner = (
                goal * CORES_HERE
                + (1 - spare) * j
                + spare * (CORES * (goal % PAIR) + CORES - 1)
            )
            columns = block(goal * per_level + j, HEAD_DIM)
            if index == 0:
                moves = [
                    (k_ref, keys_in.at[spare, my_rows, :], kv_sem.at[0, spare]),
                    (v_ref, values_in.at[spare, my_rows, :], kv_sem.at[1, spare]),
                ]
            else:
                moves = [
                    (q_ref, queries.at[spare, my_rows, :], q_sem.at[spare, me]),
                    (g_ref, grads.at[spare, my_rows, :], g_sem.at[spare, me]),
                ]

            @pl.when(owner != me)
            def _():
                for n, (src, dst, got) in enumerate(moves):
                    remote(src.at[:, columns], dst, send_in.at[2 * index + n], got, owner).start()

            @pl.when(owner == me)
            def _():
                for n, (src, dst, got) in enumerate(moves):
                    arrived = own_sem.at[n, spare] if index == 0 else got
                    pltpu.make_async_copy(src.at[:, columns], dst, arrived).start()

            return carry

        lax.fori_loop(start, end, step, 0)

    chosen = pltpu.make_async_copy(chosen_ref, place_ref, chosen_sem)
    chosen.start()
    early = near * 2 * per_level
    send_pair(0, 0, early)

    @pl.when(near == 1)
    def _():
        pl.semaphore_wait(barrier, group)

    send_pair(0, early, HEADS)
    send_pair(1, 0, HEADS)
    chosen.wait()

    def find(t, carry):
        for u in range(devices):
            at = SEL
            for j in range(SEL):
                at = jnp.where(place_ref[j, t] == u, j, at)
            spot[t, u] = at
        return carry

    lax.fori_loop(0, devices, find, 0)

    for i in range(CORES_HERE):
        kept[i, SEL] = jnp.zeros((TILE, 2 * HEAD_DIM), jnp.bfloat16)

    def send_back(slot, tile, moves):
        @pl.when(tile != me)
        def _():
            for a, src, dst in moves:
                remote(src, dst, send_out.at[a, slot], back_sem.at[a], tile).start()

        @pl.when(tile == me)
        def _():
            for a, src, dst in moves:
                pltpu.make_async_copy(src, dst, own_out.at[a, slot]).start()

    def run_head(slot, carry):
        head = level * per_level + (1 - slot) * (me % CORES_HERE) + slot * CORES_HERE
        columns = block(head, HEAD_DIM)

        def send_rows(tile):
            rows = block(tile, TILE)
            send_back(
                slot,
                tile,
                [
                    (0, out_o.at[slot, rows, :], ro_ref.at[:, columns]),
                    (1, out_q.at[slot, rows, :], rq_ref.at[:, columns]),
                ],
            )

        for n, (source, turned, turned_pool) in enumerate(
            ((keys_in, keys_t, keys_pool), (values_in, values_t, values_pool))
        ):
            wait_for(source.at[slot, pl.ds(0, tokens - TILE), :], kv_sem.at[n, slot])
            wait_for(source.at[slot, my_rows, :], own_sem.at[n, slot])
            part = slice(n * HEAD_DIM, (n + 1) * HEAD_DIM)
            rows = source[slot]
            means = jnp.sum(rows.astype(jnp.float32).reshape(pools, POOL, HEAD_DIM), axis=1)
            means = (means * (1.0 / POOL)).astype(jnp.bfloat16)
            joined_pool[:, part] = means
            turned_pool[...] = means.T
            for tile in range(devices):
                one = rows[tile * TILE : (tile + 1) * TILE]
                joined[tile, :, part] = one
                turned[tile] = one.T
        total[...] = jnp.zeros_like(total)

        def tile_step(n, carry):
            i = lax.rem(n, CORES_HERE)
            t = level_at(n // CORES_HERE) * CORES_HERE + i
            rows = block(t, TILE)

            @pl.when(n > 0)
            def _():
                before = n - 1
                send_rows(
                    level_at(before // CORES_HERE) * CORES_HERE + lax.rem(before, CORES_HERE)
                )

            wait_for(queries.at[slot, rows, :], q_sem.at[slot, t])
            wait_for(grads.at[slot, rows, :], g_sem.at[slot, t])
            query = queries[slot, rows, :]
            grad = grads[slot, rows, :]
            blank = jnp.zeros_like(query)
            paired = jnp.concatenate(
                [
                    jnp.concatenate([query, blank], axis=1),
                    jnp.concatenate([blank, grad], axis=1),
                ],
                axis=0,
            )
            pairs[i] = paired
            places = [place_ref[j, t] for j in range(SEL)]
            listed = jnp.concatenate(
                [joined[place] for place in places] + [joined_pool[...]], axis=0
            )
            both = contract(listed, paired, 1, 1)
            scores = both[:, :TILE]
            prob_grad = both[:, TILE:]
            summit = jnp.max(scores, axis=0, keepdims=True)
            raised = jnp.exp2((scores - summit) * rate)
            scale = 1.0 / jnp.sum(raised, axis=0, keepdims=True)
            dots = jnp.sum(raised * prob_grad, axis=0, keepdims=True) * scale
            weights = raised * scale
            score_grad = (weights * (prob_grad - dots)).astype(jnp.bfloat16)
            rounded = weights.astype(jnp.bfloat16)
            for part, values in ((0, score_grad), (HEAD_DIM, rounded)):
                for j in range(SEL):
                    kept[i, j, :, part : part + HEAD_DIM] = values[j * TILE : (j + 1) * TILE]
                kept_pool[i, :, part : part + HEAD_DIM] = values[listed_rows:]
            listed_kt = jnp.concatenate(
                [keys_t[place] for place in places] + [keys_pool[...]], axis=1
            )
            listed_vt = jnp.concatenate(
                [values_t[place] for place in places] + [values_pool[...]], axis=1
            )
            out_t = jnp.dot(listed_vt, rounded, preferred_element_type=jnp.float32)
            dq_t = jnp.dot(listed_kt, score_grad, preferred_element_type=jnp.float32) * scaling
            out_o[slot, rows, :] = out_t.T.astype(jnp.bfloat16)
            out_q[slot, rows, :] = dq_t.T.astype(jnp.bfloat16)
            return carry

        def add_terms(g, carry):
            first = level_at(g) * CORES_HERE
            facing = pairs[...].reshape(CORES_HERE * 2 * TILE, 2 * HEAD_DIM)
            for u in range(devices):
                found = jnp.concatenate(
                    [kept[i, spot[first + i, u]] for i in range(CORES_HERE)],
                    axis=1,
                )
                total[u * TILE : (u + 1) * TILE, :] += jnp.dot(
                    found, facing, preferred_element_type=jnp.float32
                )
            found = jnp.concatenate([kept_pool[i] for i in range(CORES_HERE)], axis=1)
            total[tokens:, :] += jnp.dot(found, facing, preferred_element_type=jnp.float32)
            return carry

        def group_step(g, carry):
            lax.fori_loop(g * CORES_HERE, (g + 1) * CORES_HERE, tile_step, 0)
            return add_terms(g, carry)

        lax.fori_loop(0, levels, group_step, 0)
        send_rows(level_at(levels - 1) * CORES_HERE + CORES_HERE - 1)
        for ref, at, factor in ((out_k, 0, scaling), (out_v, HEAD_DIM, 1.0)):
            coarse = total[tokens:, at : at + HEAD_DIM] * factor
            fine = total[:tokens, at : at + HEAD_DIM] * factor
            fine = fine.reshape(pools, POOL, HEAD_DIM) + (coarse * (1.0 / POOL))[:, None, :]
            ref[slot] = fine.reshape(tokens, HEAD_DIM).astype(jnp.bfloat16)
            start = 0 if at == 0 else per_tile
            for tile in range(devices):
                out_c[slot, tile, start : start + per_tile, :] = coarse[
                    tile * per_tile : (tile + 1) * per_tile
                ]

        def send_sums(n, carry):
            tile = level_at(levels - 1 - n // CORES_HERE) * CORES_HERE + lax.rem(n, CORES_HERE)
            rows = block(tile, TILE)
            send_back(
                slot,
                tile,
                [
                    (2, out_k.at[slot, rows, :], rk_ref.at[:, columns]),
                    (3, out_v.at[slot, rows, :], rv_ref.at[:, columns]),
                    (4, out_c.at[slot, tile], rc_ref.at[head]),
                ],
            )
            return carry

        lax.fori_loop(0, devices, send_sums, 0)
        return carry

    lax.fori_loop(0, count, run_head, 0)

    stores = (out_o, out_q, out_k, out_v)
    landed = (ro_ref, rq_ref, rk_ref, rv_ref)

    def sent(slot):
        for a, ref in enumerate(stores):
            wait_for(ref.at[slot, pl.ds(0, tokens - TILE), :], send_out.at[a, slot])
            wait_for(ref.at[slot, my_rows, :], own_out.at[a, slot])
        wait_for(out_c.at[slot, pl.ds(0, devices - 1)], send_out.at[4, slot])
        wait_for(out_c.at[slot, me], own_out.at[4, slot])

    def finish(own):
        for n, ref in enumerate((k_ref, v_ref, q_ref, g_ref)):
            wait_for(ref.at[:, pl.ds(0, (HEADS - own) * HEAD_DIM)], send_in.at[n])
        for a, ref in enumerate(landed):
            wait_for(ref.at[:, pl.ds(0, (HEADS - own) * HEAD_DIM)], back_sem.at[a])
        wait_for(rc_ref.at[pl.ds(0, HEADS - own)], back_sem.at[4])

    sent(0)

    @pl.when(two)
    def _():
        sent(1)
        finish(2)

    @pl.when(jnp.logical_not(two))
    def _():
        finish(1)


def fused(selected, arrays, devices):
    turned_list, *arrays = (
        pltpu.with_memory_space_constraint(part, pltpu.HBM) for part in (selected.T, *arrays)
    )
    tokens = devices * TILE
    pools = tokens // POOL
    flat = pltpu.VMEM((TILE, HEADS * HEAD_DIM), jnp.bfloat16)
    coarse = jax.ShapeDtypeStruct((HEADS, 2 * TILE // POOL, HEAD_DIM), jnp.float32)
    slabs = pltpu.VMEM((SLOTS, tokens, HEAD_DIM), jnp.bfloat16)
    turned = pltpu.VMEM((devices, HEAD_DIM, TILE), jnp.bfloat16)
    turned_pool = pltpu.VMEM((HEAD_DIM, pools), jnp.bfloat16)
    return pl.pallas_call(
        functools.partial(fused_kernel, devices),
        out_shape=[flat] * 4 + [coarse],
        in_specs=[pl.BlockSpec(memory_space=pltpu.HBM)] * 5,
        out_specs=[pl.BlockSpec(memory_space=pltpu.VMEM)] * 4
        + [pl.BlockSpec(memory_space=pl.ANY)],
        scratch_shapes=[
            slabs,
            slabs,
            slabs,
            slabs,
            slabs,
            slabs,
            slabs,
            slabs,
            pltpu.VMEM((SLOTS, devices, 2 * TILE // POOL, HEAD_DIM), jnp.float32),
            pltpu.VMEM((devices, TILE, 2 * HEAD_DIM), jnp.bfloat16),
            pltpu.VMEM((pools, 2 * HEAD_DIM), jnp.bfloat16),
            turned,
            turned_pool,
            turned,
            turned_pool,
            pltpu.VMEM((CORES_HERE, 2 * TILE, 2 * HEAD_DIM), jnp.bfloat16),
            pltpu.VMEM((CORES_HERE, SEL + 1, TILE, 2 * HEAD_DIM), jnp.bfloat16),
            pltpu.VMEM((CORES_HERE, pools, 2 * HEAD_DIM), jnp.bfloat16),
            pltpu.VMEM((tokens + pools, 2 * HEAD_DIM), jnp.float32),
            pltpu.SMEM(turned_list.shape, jnp.int32),
            pltpu.SMEM((devices, devices), jnp.int32),
            pltpu.SemaphoreType.DMA,
            pltpu.SemaphoreType.DMA((4,)),
            pltpu.SemaphoreType.DMA((2, SLOTS)),
            pltpu.SemaphoreType.DMA((2, SLOTS)),
            pltpu.SemaphoreType.DMA((SLOTS, devices)),
            pltpu.SemaphoreType.DMA((SLOTS, devices)),
            pltpu.SemaphoreType.DMA((5, SLOTS)),
            pltpu.SemaphoreType.DMA((5,)),
            pltpu.SemaphoreType.DMA((5, SLOTS)),
        ],
        compiler_params=pltpu.CompilerParams(
            collective_id=0, has_side_effects=True, vmem_limit_bytes=40 * 2**20
        ),
        name="exchange_heads",
    )(turned_list, *arrays)


def place_kernel(a_ref, b_ref, c_ref, d_ref, coarse_ref,
                 oa_ref, ob_ref, oc_ref, od_ref, keys_ref, values_ref, sem):
    moves = [
        pltpu.make_async_copy(source, target, sem.at[n])
        for n, (source, target) in enumerate(
            zip((a_ref, b_ref, c_ref, d_ref), (oa_ref, ob_ref, oc_ref, od_ref))
        )
    ]
    for move in moves:
        move.start()
    per_tile = TILE // POOL
    for head in range(HEADS):
        columns = slice(head * HEAD_DIM, (head + 1) * HEAD_DIM)
        keys_ref[:, columns] = coarse_ref[head, :per_tile]
        values_ref[:, columns] = coarse_ref[head, per_tile:]
    for move in moves:
        move.wait()


def place(parts, coarse):
    shape = jax.ShapeDtypeStruct(parts[0].shape, jnp.bfloat16)
    sums = jax.ShapeDtypeStruct((TILE // POOL, HEADS * HEAD_DIM), jnp.float32)
    whole = pl.BlockSpec(memory_space=pltpu.VMEM)
    parts = [pltpu.with_memory_space_constraint(part, pltpu.VMEM) for part in parts]
    return pl.pallas_call(
        place_kernel,
        out_shape=[shape] * 4 + [sums] * 2,
        in_specs=[whole] * 5,
        out_specs=[pl.BlockSpec(memory_space=pl.ANY)] * 4 + [whole] * 2,
        scratch_shapes=[pltpu.SemaphoreType.DMA((4,))],
        compiler_params=pltpu.CompilerParams(vmem_limit_bytes=2**23),
        name="place",
    )(*parts, coarse)


def exchange_shards(query_rows, key_rows, value_rows, out_grad, selected):
    devices = lax.axis_size("ctx")
    *parts, coarse = fused(selected, (key_rows, value_rows, query_rows, out_grad), devices)
    return tuple(place(parts, coarse))


def shards(query_rows, key_rows, value_rows, out_grad, selected):
    devices = lax.axis_size("ctx")
    fits = devices == 4 * CORES * PAIR and query_rows.shape[0] == TILE
    chosen = exchange_shards if fits else listed_shards
    return chosen(query_rows, key_rows, value_rows, out_grad, selected)


def solution(mesh):
    in_specs = (
        P(("groups", "ctx"), None),
        P(("groups", "ctx"), None),
        P(("groups", "ctx"), None),
        P(("groups", "ctx"), None),
        P("groups", None),
    )
    out_specs = (
        P(("groups", "ctx"), None),
        P(("groups", "ctx"), None),
        P(("groups", "ctx"), None),
        P(("groups", "ctx"), None),
        P(("groups", "ctx"), None),
        P(("groups", "ctx"), None),
    )
    return jax.shard_map(shards, mesh=mesh, in_specs=in_specs, out_specs=out_specs, check_vma=False)
```

```python
import functools
import math

import jax
import jax.numpy as jnp
from jax import lax
from jax.experimental import pallas as pl
from jax.experimental.pallas import tpu as pltpu
from jax.sharding import PartitionSpec as P

HEADS = 20
HEAD_DIM = 128
TILE = 128
POOL = 64
SEL = 8
CORES = 2
PAIR = 2


def pooled(rows):
    return jnp.mean(rows.astype(jnp.float32).reshape(-1, POOL, rows.shape[1]), axis=1).astype(
        jnp.bfloat16
    )


def contract(left, right, left_dim, right_dim):
    return lax.dot_general(
        left, right, (((left_dim,), (right_dim,)), ((), ())), preferred_element_type=jnp.float32
    )


def attend(queries, grads_out, keys_all, values_all):
    scaling = HEAD_DIM ** (-0.5)
    out_parts, query_parts, key_parts, value_parts = ([], [], [], [])
    for head in range(HEADS):
        lower = head * HEAD_DIM
        upper = lower + HEAD_DIM
        head_query = queries[:, lower:upper]
        head_grad = grads_out[:, lower:upper]
        head_key = keys_all[:, lower:upper]
        head_value = values_all[:, lower:upper]
        scores = contract(head_query, head_key, 1, 1) * scaling
        summit = jnp.max(scores, axis=-1, keepdims=True)
        raised = jnp.exp(scores - summit)
        weights = raised / jnp.sum(raised, axis=-1, keepdims=True)
        rounded = weights.astype(jnp.bfloat16)
        out_rows = jnp.dot(rounded, head_value, preferred_element_type=jnp.float32).astype(
            jnp.bfloat16
        )
        row_dots = jnp.sum(
            head_grad.astype(jnp.float32) * out_rows.astype(jnp.float32), axis=-1, keepdims=True
        )
        prob_grad = contract(head_grad, head_value, 1, 1)
        score_grad = (weights * (prob_grad - row_dots)).astype(jnp.bfloat16)
        query_grad = jnp.dot(score_grad, head_key, preferred_element_type=jnp.float32) * scaling
        key_terms = contract(score_grad, head_query, 0, 0) * scaling
        value_terms = contract(rounded, head_grad, 0, 0)
        out_parts.append(out_rows)
        query_parts.append(query_grad.astype(jnp.bfloat16))
        key_parts.append(key_terms)
        value_parts.append(value_terms)
    return (
        jnp.concatenate(out_parts, axis=1),
        jnp.concatenate(query_parts, axis=1),
        jnp.concatenate(key_parts, axis=1),
        jnp.concatenate(value_parts, axis=1),
    )


def package(tiles_in, pooled_in, devices, spread):
    tiles_here, tile_len, columns = tiles_in.shape
    per_tile = tile_len // POOL
    split_rows = tiles_in.reshape(tiles_here, devices, spread, columns)
    copies = jnp.broadcast_to(
        pooled_in.reshape(tiles_here, 1, per_tile, columns),
        (tiles_here, devices, per_tile, columns),
    )
    return jnp.concatenate([split_rows, copies], axis=2).reshape(
        tiles_here, devices * (spread + per_tile), columns
    )


def listed_shards(query_rows, key_rows, value_rows, out_grad, selected):
    height, columns = query_rows.shape
    devices = lax.axis_size("ctx")
    tiles_here = height // TILE
    spread = TILE // devices
    own_keys = pooled(key_rows)
    own_values = pooled(value_rows)
    key_tiles = key_rows.reshape(tiles_here, TILE, columns)
    value_tiles = value_rows.reshape(tiles_here, TILE, columns)
    joined_keys, joined_values = (
        lax.all_to_all(
            package(key_tiles, own_keys, devices, spread),
            "ctx",
            split_axis=1,
            concat_axis=0,
            tiled=True,
        ),
        lax.all_to_all(
            package(value_tiles, own_values, devices, spread),
            "ctx",
            split_axis=1,
            concat_axis=0,
            tiled=True,
        ),
    )
    held_keys = joined_keys[:, :spread]
    held_values = joined_values[:, :spread]
    pool_keys = joined_keys[:, spread:].reshape(-1, columns)
    pool_values = joined_values[:, spread:].reshape(-1, columns)
    comp_count = pool_keys.shape[0]
    got_keys, got_values = (
        lax.all_to_all(held_keys[selected], "ctx", split_axis=0, concat_axis=2, tiled=True),
        lax.all_to_all(held_values[selected], "ctx", split_axis=0, concat_axis=2, tiled=True),
    )
    fine_keys = got_keys.reshape(tiles_here, SEL * TILE, columns)
    fine_values = got_values.reshape(tiles_here, SEL * TILE, columns)
    out_tiles, query_tiles, key_listed, value_listed = ([], [], [], [])
    keys_all = jnp.concatenate([pool_keys, fine_keys[0]], axis=0)
    values_all = jnp.concatenate([pool_values, fine_values[0]], axis=0)
    out_rows, query_grad, key_terms, value_terms = attend(
        query_rows, out_grad, keys_all, values_all
    )
    out_tiles.append(out_rows)
    query_tiles.append(query_grad)
    coarse_keys = key_terms[:comp_count]
    coarse_values = value_terms[:comp_count]
    key_listed.append(key_terms[comp_count:].astype(jnp.bfloat16))
    value_listed.append(value_terms[comp_count:].astype(jnp.bfloat16))
    own_coarse_keys, own_coarse_values = (
        lax.psum_scatter(coarse_keys, "ctx", scatter_dimension=0, tiled=True),
        lax.psum_scatter(coarse_values, "ctx", scatter_dimension=0, tiled=True),
    )
    listed_keys = jnp.stack(key_listed).reshape(tiles_here * SEL, devices, spread, columns)
    listed_values = jnp.stack(value_listed).reshape(tiles_here * SEL, devices, spread, columns)
    back_keys, back_values = (
        lax.all_to_all(listed_keys, "ctx", split_axis=1, concat_axis=0, tiled=True),
        lax.all_to_all(listed_values, "ctx", split_axis=1, concat_axis=0, tiled=True),
    )
    tile_ids = jnp.arange(selected.shape[0], dtype=jnp.int32)[:, None]
    member = (selected.reshape(1, -1) == tile_ids).astype(jnp.bfloat16)
    entries = member.shape[1]
    sum_keys = jnp.dot(
        member, back_keys.reshape(entries, spread * columns), preferred_element_type=jnp.float32
    )
    sum_values = jnp.dot(
        member, back_values.reshape(entries, spread * columns), preferred_element_type=jnp.float32
    )
    held_key_grad = sum_keys.astype(jnp.bfloat16).reshape(devices, tiles_here, spread, columns)
    held_value_grad = sum_values.astype(jnp.bfloat16).reshape(devices, tiles_here, spread, columns)
    owned_keys, owned_values = (
        lax.all_to_all(held_key_grad, "ctx", split_axis=0, concat_axis=2, tiled=True),
        lax.all_to_all(held_value_grad, "ctx", split_axis=0, concat_axis=2, tiled=True),
    )
    grad_key = (
        owned_keys.reshape(height, columns).astype(jnp.float32)
        + jnp.repeat(own_coarse_keys, POOL, axis=0) / POOL
    ).astype(jnp.bfloat16)
    grad_value = (
        owned_values.reshape(height, columns).astype(jnp.float32)
        + jnp.repeat(own_coarse_values, POOL, axis=0) / POOL
    ).astype(jnp.bfloat16)
    attended = out_tiles[0]
    grad_query = query_tiles[0]
    return (attended, grad_query, grad_key, grad_value, own_coarse_keys, own_coarse_values)


SLOTS = 2
CORES_HERE = CORES * PAIR


def remote(src, dst, sent, got, target):
    return pltpu.make_async_remote_copy(
        src_ref=src,
        dst_ref=dst,
        send_sem=sent,
        recv_sem=got,
        device_id={"ctx": target},
        device_id_type=pl.DeviceIdType.MESH,
    )


def wait_for(ref, semaphore):
    pltpu.make_async_copy(ref, ref, semaphore).wait()


def block(index, size):
    return pl.ds(pl.multiple_of(index * size, size), size)


def greet(target):
    pl.semaphore_signal(
        pltpu.get_barrier_semaphore(),
        inc=1,
        device_id={"ctx": target},
        device_id_type=pl.DeviceIdType.MESH,
    )


def fused_kernel(devices, chosen_ref, k_ref, v_ref, q_ref, g_ref,
                 ro_ref, rq_ref, rk_ref, rv_ref, rc_ref,
                 keys_in, values_in, queries, grads, out_o, out_q, out_k, out_v, out_c,
                 joined, joined_pool, keys_t, keys_pool, values_t, values_pool, pairs, kept,
                 kept_pool, total, place_ref, spot, chosen_sem,
                 send_in, kv_sem, own_sem, q_sem, g_sem, send_out, back_sem, own_out):
    me = lax.axis_index("ctx")
    levels = devices // CORES_HERE
    per_level = HEADS // levels
    tokens = devices * TILE
    pools = tokens // POOL
    per_tile = TILE // POOL
    listed_rows = SEL * TILE
    level = me // CORES_HERE
    upper = level // 2
    near = (1 - upper) * level + upper * (levels - 1 - level)
    extra_at = CORES * (level % PAIR) + CORES - 1
    two = me % CORES_HERE == extra_at
    apart = me % CORES_HERE - extra_at
    count = 1 + (CORES_HERE * CORES_HERE - apart * apart) // (CORES_HERE * CORES_HERE)
    scaling = HEAD_DIM ** (-0.5)
    rate = scaling * math.log2(math.e)

    def level_at(step):
        turn = step + near * (1 - 3 * (step // 2) + 2 * (step // 3))
        return (1 - upper) * turn + upper * (levels - 1 - turn)

    barrier = pltpu.get_barrier_semaphore()
    place_here = me % CORES_HERE
    facing_level = levels - 1 - level
    for k in range(CORES_HERE):
        if k:
            greet(level * CORES_HERE + lax.rem(place_here + k, CORES_HERE))
        greet(facing_level * CORES_HERE + k)
    group = 2 * CORES_HERE
    others = [(1 - near) * (1 + up) + near * (levels - 1) * up for up in range(2)]

    @pl.when(near == 1)
    def _():
        pl.semaphore_wait(barrier, group - 1)

    @pl.when(near == 0)
    def _():
        pl.semaphore_wait(barrier, devices - 1)

    for up in range(2):
        for k in range(CORES_HERE):
            greet(others[up] * CORES_HERE + k)

    my_rows = block(me, TILE)

    def send_pair(index, start, end):
        def step(i, carry):
            goal = level_at(i // per_level)
            j = lax.rem(i + me, per_level)
            spare = j // CORES_HERE
            owner = (
                goal * CORES_HERE
                + (1 - spare) * j
                + spare * (CORES * (goal % PAIR) + CORES - 1)
            )
            columns = block(goal * per_level + j, HEAD_DIM)
            if index == 0:
                moves = [
                    (k_ref, keys_in.at[spare, my_rows, :], kv_sem.at[0, spare]),
                    (v_ref, values_in.at[spare, my_rows, :], kv_sem.at[1, spare]),
                ]
            else:
                moves = [
                    (q_ref, queries.at[spare, my_rows, :], q_sem.at[spare, me]),
                    (g_ref, grads.at[spare, my_rows, :], g_sem.at[spare, me]),
                ]

            @pl.when(owner != me)
            def _():
                for n, (src, dst, got) in enumerate(moves):
                    remote(src.at[:, columns], dst, send_in.at[2 * index + n], got, owner).start()

            @pl.when(owner == me)
            def _():
                for n, (src, dst, got) in enumerate(moves):
                    arrived = own_sem.at[n, spare] if index == 0 else got
                    pltpu.make_async_copy(src.at[:, columns], dst, arrived).start()

            return carry

        lax.fori_loop(start, end, step, 0)

    chosen = pltpu.make_async_copy(chosen_ref, place_ref, chosen_sem)
    chosen.start()
    early = near * 2 * per_level
    send_pair(0, 0, early)

    @pl.when(near == 1)
    def _():
        pl.semaphore_wait(barrier, group)

    send_pair(0, early, HEADS)
    send_pair(1, 0, HEADS)
    chosen.wait()

    def find(t, carry):
        for u in range(devices):
            at = SEL
            for j in range(SEL):
                at = jnp.where(place_ref[j, t] == u, j, at)
            spot[t, u] = at
        return carry

    lax.fori_loop(0, devices, find, 0)

    for i in range(CORES_HERE):
        kept[i, SEL] = jnp.zeros((TILE, 2 * HEAD_DIM), jnp.bfloat16)

    def send_back(slot, tile, moves):
        @pl.when(tile != me)
        def _():
            for a, src, dst in moves:
                remote(src, dst, send_out.at[a, slot], back_sem.at[a], tile).start()

        @pl.when(tile == me)
        def _():
            for a, src, dst in moves:
                pltpu.make_async_copy(src, dst, own_out.at[a, slot]).start()

    def run_head(slot, carry):
        head = level * per_level + (1 - slot) * (me % CORES_HERE) + slot * CORES_HERE
        columns = block(head, HEAD_DIM)

        def send_rows(tile):
            rows = block(tile, TILE)
            send_back(
                slot,
                tile,
                [
                    (0, out_o.at[slot, rows, :], ro_ref.at[:, columns]),
                    (1, out_q.at[slot, rows, :], rq_ref.at[:, columns]),
                ],
            )

        for n, (source, turned, turned_pool) in enumerate(
            ((keys_in, keys_t, keys_pool), (values_in, values_t, values_pool))
        ):
            wait_for(source.at[slot, pl.ds(0, tokens - TILE), :], kv_sem.at[n, slot])
            wait_for(source.at[slot, my_rows, :], own_sem.at[n, slot])
            part = slice(n * HEAD_DIM, (n + 1) * HEAD_DIM)
            rows = source[slot]
            means = jnp.sum(rows.astype(jnp.float32).reshape(pools, POOL, HEAD_DIM), axis=1)
            means = (means * (1.0 / POOL)).astype(jnp.bfloat16)
            joined_pool[:, part] = means
            turned_pool[...] = means.T
            for tile in range(devices):
                one = rows[tile * TILE : (tile + 1) * TILE]
                joined[tile, :, part] = one
                turned[tile] = one.T
        total[...] = jnp.zeros_like(total)

        def tile_step(n, carry):
            i = lax.rem(n, CORES_HERE)
            t = level_at(n // CORES_HERE) * CORES_HERE + i
            rows = block(t, TILE)

            @pl.when(n > 0)
            def _():
                before = n - 1
                send_rows(
                    level_at(before // CORES_HERE) * CORES_HERE + lax.rem(before, CORES_HERE)
                )

            wait_for(queries.at[slot, rows, :], q_sem.at[slot, t])
            wait_for(grads.at[slot, rows, :], g_sem.at[slot, t])
            query = queries[slot, rows, :]
            grad = grads[slot, rows, :]
            blank = jnp.zeros_like(query)
            paired = jnp.concatenate(
                [
                    jnp.concatenate([query, blank], axis=1),
                    jnp.concatenate([blank, grad], axis=1),
                ],
                axis=0,
            )
            pairs[i] = paired
            places = [place_ref[j, t] for j in range(SEL)]
            listed = jnp.concatenate(
                [joined[place] for place in places] + [joined_pool[...]], axis=0
            )
            both = contract(listed, paired, 1, 1)
            scores = both[:, :TILE]
            prob_grad = both[:, TILE:]
            summit = jnp.max(scores, axis=0, keepdims=True)
            raised = jnp.exp2((scores - summit) * rate)
            scale = 1.0 / jnp.sum(raised, axis=0, keepdims=True)
            weights = raised * scale
            rounded = weights.astype(jnp.bfloat16)
            dots = jnp.sum(rounded.astype(jnp.float32) * prob_grad, axis=0, keepdims=True)
            score_grad = (weights * (prob_grad - dots)).astype(jnp.bfloat16)
            for part, values in ((0, score_grad), (HEAD_DIM, rounded)):
                for j in range(SEL):
                    kept[i, j, :, part : part + HEAD_DIM] = values[j * TILE : (j + 1) * TILE]
                kept_pool[i, :, part : part + HEAD_DIM] = values[listed_rows:]
            listed_kt = jnp.concatenate(
                [keys_t[place] for place in places] + [keys_pool[...]], axis=1
            )
            listed_vt = jnp.concatenate(
                [values_t[place] for place in places] + [values_pool[...]], axis=1
            )
            out_t = jnp.dot(listed_vt, rounded, preferred_element_type=jnp.float32)
            dq_t = jnp.dot(listed_kt, score_grad, preferred_element_type=jnp.float32) * scaling
            out_o[slot, rows, :] = out_t.T.astype(jnp.bfloat16)
            out_q[slot, rows, :] = dq_t.T.astype(jnp.bfloat16)
            return carry

        def add_terms(g, carry):
            first = level_at(g) * CORES_HERE
            facing = pairs[...].reshape(CORES_HERE * 2 * TILE, 2 * HEAD_DIM)
            for u in range(devices):
                found = jnp.concatenate(
                    [kept[i, spot[first + i, u]] for i in range(CORES_HERE)],
                    axis=1,
                )
                total[u * TILE : (u + 1) * TILE, :] += jnp.dot(
                    found, facing, preferred_element_type=jnp.float32
                )
            found = jnp.concatenate([kept_pool[i] for i in range(CORES_HERE)], axis=1)
            total[tokens:, :] += jnp.dot(found, facing, preferred_element_type=jnp.float32)
            return carry

        def group_step(g, carry):
            lax.fori_loop(g * CORES_HERE, (g + 1) * CORES_HERE, tile_step, 0)
            return add_terms(g, carry)

        lax.fori_loop(0, levels, group_step, 0)
        send_rows(level_at(levels - 1) * CORES_HERE + CORES_HERE - 1)
        for ref, at, factor in ((out_k, 0, scaling), (out_v, HEAD_DIM, 1.0)):
            coarse = total[tokens:, at : at + HEAD_DIM] * factor
            fine = total[:tokens, at : at + HEAD_DIM] * factor
            fine = fine.reshape(pools, POOL, HEAD_DIM) + (coarse * (1.0 / POOL))[:, None, :]
            ref[slot] = fine.reshape(tokens, HEAD_DIM).astype(jnp.bfloat16)
            start = 0 if at == 0 else per_tile
            for tile in range(devices):
                out_c[slot, tile, start : start + per_tile, :] = coarse[
                    tile * per_tile : (tile + 1) * per_tile
                ]

        def send_sums(n, carry):
            goal = level_at(levels - 1 - n // CORES_HERE)
            tile = goal * CORES_HERE + lax.rem(n + me, CORES_HERE)
            rows = block(tile, TILE)
            send_back(
                slot,
                tile,
                [
                    (2, out_k.at[slot, rows, :], rk_ref.at[:, columns]),
                    (3, out_v.at[slot, rows, :], rv_ref.at[:, columns]),
                    (4, out_c.at[slot, tile], rc_ref.at[head]),
                ],
            )
            return carry

        lax.fori_loop(0, devices, send_sums, 0)
        return carry

    lax.fori_loop(0, count, run_head, 0)

    stores = (out_o, out_q, out_k, out_v)
    landed = (ro_ref, rq_ref, rk_ref, rv_ref)

    def sent(slot):
        for a, ref in enumerate(stores):
            wait_for(ref.at[slot, pl.ds(0, tokens - TILE), :], send_out.at[a, slot])
            wait_for(ref.at[slot, my_rows, :], own_out.at[a, slot])
        wait_for(out_c.at[slot, pl.ds(0, devices - 1)], send_out.at[4, slot])
        wait_for(out_c.at[slot, me], own_out.at[4, slot])

    def finish(own):
        for n, ref in enumerate((k_ref, v_ref, q_ref, g_ref)):
            wait_for(ref.at[:, pl.ds(0, (HEADS - own) * HEAD_DIM)], send_in.at[n])
        for a, ref in enumerate(landed):
            wait_for(ref.at[:, pl.ds(0, (HEADS - own) * HEAD_DIM)], back_sem.at[a])
        wait_for(rc_ref.at[pl.ds(0, HEADS - own)], back_sem.at[4])

    sent(0)

    @pl.when(two)
    def _():
        sent(1)
        finish(2)

    @pl.when(jnp.logical_not(two))
    def _():
        finish(1)


def fused(selected, arrays, devices):
    turned_list, *arrays = (
        pltpu.with_memory_space_constraint(part, pltpu.HBM) for part in (selected.T, *arrays)
    )
    tokens = devices * TILE
    pools = tokens // POOL
    flat = pltpu.VMEM((TILE, HEADS * HEAD_DIM), jnp.bfloat16)
    coarse = jax.ShapeDtypeStruct((HEADS, 2 * TILE // POOL, HEAD_DIM), jnp.float32)
    slabs = pltpu.VMEM((SLOTS, tokens, HEAD_DIM), jnp.bfloat16)
    turned = pltpu.VMEM((devices, HEAD_DIM, TILE), jnp.bfloat16)
    turned_pool = pltpu.VMEM((HEAD_DIM, pools), jnp.bfloat16)
    return pl.pallas_call(
        functools.partial(fused_kernel, devices),
        out_shape=[flat] * 4 + [coarse],
        in_specs=[pl.BlockSpec(memory_space=pltpu.HBM)] * 5,
        out_specs=[pl.BlockSpec(memory_space=pltpu.VMEM)] * 4
        + [pl.BlockSpec(memory_space=pl.ANY)],
        scratch_shapes=[
            slabs,
            slabs,
            slabs,
            slabs,
            slabs,
            slabs,
            slabs,
            slabs,
            pltpu.VMEM((SLOTS, devices, 2 * TILE // POOL, HEAD_DIM), jnp.float32),
            pltpu.VMEM((devices, TILE, 2 * HEAD_DIM), jnp.bfloat16),
            pltpu.VMEM((pools, 2 * HEAD_DIM), jnp.bfloat16),
            turned,
            turned_pool,
            turned,
            turned_pool,
            pltpu.VMEM((CORES_HERE, 2 * TILE, 2 * HEAD_DIM), jnp.bfloat16),
            pltpu.VMEM((CORES_HERE, SEL + 1, TILE, 2 * HEAD_DIM), jnp.bfloat16),
            pltpu.VMEM((CORES_HERE, pools, 2 * HEAD_DIM), jnp.bfloat16),
            pltpu.VMEM((tokens + pools, 2 * HEAD_DIM), jnp.float32),
            pltpu.SMEM(turned_list.shape, jnp.int32),
            pltpu.SMEM((devices, devices), jnp.int32),
            pltpu.SemaphoreType.DMA,
            pltpu.SemaphoreType.DMA((4,)),
            pltpu.SemaphoreType.DMA((2, SLOTS)),
            pltpu.SemaphoreType.DMA((2, SLOTS)),
            pltpu.SemaphoreType.DMA((SLOTS, devices)),
            pltpu.SemaphoreType.DMA((SLOTS, devices)),
            pltpu.SemaphoreType.DMA((5, SLOTS)),
            pltpu.SemaphoreType.DMA((5,)),
            pltpu.SemaphoreType.DMA((5, SLOTS)),
        ],
        compiler_params=pltpu.CompilerParams(
            collective_id=0, has_side_effects=True, vmem_limit_bytes=40 * 2**20
        ),
        name="exchange_heads",
    )(turned_list, *arrays)


def place_kernel(a_ref, b_ref, c_ref, d_ref, coarse_ref,
                 oa_ref, ob_ref, oc_ref, od_ref, keys_ref, values_ref, sem):
    moves = [
        pltpu.make_async_copy(source, target, sem.at[n])
        for n, (source, target) in enumerate(
            zip((a_ref, b_ref, c_ref, d_ref), (oa_ref, ob_ref, oc_ref, od_ref))
        )
    ]
    for move in moves:
        move.start()
    per_tile = TILE // POOL
    for head in range(HEADS):
        columns = slice(head * HEAD_DIM, (head + 1) * HEAD_DIM)
        keys_ref[:, columns] = coarse_ref[head, :per_tile]
        values_ref[:, columns] = coarse_ref[head, per_tile:]
    for move in moves:
        move.wait()


def place(parts, coarse):
    shape = jax.ShapeDtypeStruct(parts[0].shape, jnp.bfloat16)
    sums = jax.ShapeDtypeStruct((TILE // POOL, HEADS * HEAD_DIM), jnp.float32)
    whole = pl.BlockSpec(memory_space=pltpu.VMEM)
    parts = [pltpu.with_memory_space_constraint(part, pltpu.VMEM) for part in parts]
    return pl.pallas_call(
        place_kernel,
        out_shape=[shape] * 4 + [sums] * 2,
        in_specs=[whole] * 5,
        out_specs=[pl.BlockSpec(memory_space=pl.ANY)] * 4 + [whole] * 2,
        scratch_shapes=[pltpu.SemaphoreType.DMA((4,))],
        compiler_params=pltpu.CompilerParams(vmem_limit_bytes=2**23),
        name="place",
    )(*parts, coarse)


def exchange_shards(query_rows, key_rows, value_rows, out_grad, selected):
    devices = lax.axis_size("ctx")
    *parts, coarse = fused(selected, (key_rows, value_rows, query_rows, out_grad), devices)
    return tuple(place(parts, coarse))


def shards(query_rows, key_rows, value_rows, out_grad, selected):
    devices = lax.axis_size("ctx")
    fits = devices == 4 * CORES * PAIR and query_rows.shape[0] == TILE
    chosen = exchange_shards if fits else listed_shards
    return chosen(query_rows, key_rows, value_rows, out_grad, selected)


def solution(mesh):
    in_specs = (
        P(("groups", "ctx"), None),
        P(("groups", "ctx"), None),
        P(("groups", "ctx"), None),
        P(("groups", "ctx"), None),
        P("groups", None),
    )
    out_specs = (
        P(("groups", "ctx"), None),
        P(("groups", "ctx"), None),
        P(("groups", "ctx"), None),
        P(("groups", "ctx"), None),
        P(("groups", "ctx"), None),
        P(("groups", "ctx"), None),
    )
    return jax.shard_map(shards, mesh=mesh, in_specs=in_specs, out_specs=out_specs, check_vma=False)
```
